256 devices in a mesh: rep: 128 (over x_hi, z, y, core), grp: 2 (over x_lo).
Axes of the slice: x: 4 (x_hi: 2, x_lo: 2; x = x_hi * 2 + x_lo), y: 4, z: 8, core: 2. Of those that a mesh axis runs over, the one named last changes fastest.
Arguments:
- local_params: bfloat16 [128, 2, 256, 8192], P('rep', 'grp'), may hold values from -130 to 130
- snapshot: bfloat16 [2, 256, 8192], P('grp'), may hold values from -4 to 4
- master: float32 [2, 256, 8192], P('grp', 'rep'), may hold values from -6 to 6
- momentum: float32 [2, 256, 8192], P('grp', 'rep'), may hold values from -4 to 4
Outputs:
- new_master: float32 [2, 256, 8192], P('grp', 'rep')
- new_momentum: float32 [2, 256, 8192], P('grp', 'rep')
- new_params: bfloat16 [2, 256, 8192], P('grp')
The draws below stay inside these ranges and needn't reach their ends.
All inputs are finite; a program needn't handle non-finite values.
Results may differ from the reference program's by a relative error of at most 0.001.
Values may be sent and summed in bfloat16 or wider, within the bound.
No kernel may reach another device: no remote copies, remote signals or barrier semaphores. Data moves between devices by JAX's collectives and lax.ppermute only.
A program may use at most 128 MiB of HBM per device.

```python
import jax
import jax.numpy as jnp
from jax import lax

D = 8192
ROWS = 256
REPLICAS = 128
GROUPS = 2


def rough_noise(key, shape):
    return jnp.clip(jax.random.normal(key, shape, jnp.float32), -3.0, 3.0)


def snapshot_base(key):
    key_base = jax.random.fold_in(key, 11)
    base = jnp.clip(jax.random.normal(key_base, (GROUPS, ROWS, D), jnp.float32), -4.0, 4.0)
    return base.astype(jnp.bfloat16)


def drift_scales(key):
    key_rows = jax.random.fold_in(key, 12)
    key_cols = jax.random.fold_in(key, 13)
    row_log = jax.random.uniform(key_rows, (GROUPS, ROWS, 1), jnp.float32, 0.0, 1.0) * jnp.log(10.0)
    col_span = jnp.log(10.0)
    ramp_span = jnp.log(3.0)
    col_log = jax.random.uniform(key_cols, (GROUPS, 1, D), jnp.float32, 0.0, 1.0) * col_span
    position = jnp.arange(ROWS, dtype=jnp.float32).reshape(1, ROWS, 1) / max(ROWS - 1, 1)
    group_pos = jnp.arange(GROUPS, dtype=jnp.float32).reshape(GROUPS, 1, 1) / max(GROUPS - 1, 1)
    row_factor = jnp.exp(row_log + ramp_span * position + jnp.log(3.0) * group_pos)
    return row_factor * jnp.exp(col_log)


def draw_snapshot(key, part):
    return snapshot_base(key)


def draw_local_params(key, part):
    start = snapshot_base(key).astype(jnp.float32)
    scale = drift_scales(key)
    common = 0.005 * rough_noise(jax.random.fold_in(key, 21), (GROUPS, ROWS, D)) * scale
    owners = jax.random.permutation(jax.random.fold_in(key, 23), REPLICAS).astype(jnp.int32)
    row_owner = (jnp.arange(ROWS, dtype=jnp.int32) // (ROWS // REPLICAS)).reshape(1, ROWS, 1)
    own_rate = 0.005
    key_own = jax.random.fold_in(key, 22)

    def one_replica(replica):
        noise = rough_noise(jax.random.fold_in(key_own, replica), (GROUPS, ROWS, D))
        spike = jnp.where(row_owner == owners[replica], 8.0, 1.0)
        return (start + common + own_rate * noise * scale * spike).astype(jnp.bfloat16)
    return lax.map(one_replica, jnp.arange(REPLICAS, dtype=jnp.int32))


def block_levels(key, extent, shards, low, largest):
    def one(dim, parts):
        steps = jax.random.uniform(jax.random.fold_in(jax.random.fold_in(key, 6), dim), (parts,), jnp.float32, low / len(shards), largest / len(shards))
        return jnp.repeat(jnp.exp(steps), extent[dim] // parts).reshape((-1,) + (1,) * (len(extent) - dim - 1))

    factor_of = one(*shards[0])
    for cut in shards[1:]:
        factor_of = factor_of * one(*cut)
    return factor_of


def scatter_about(stream_key, dims, deviation, most, cuts=(), kind=jnp.bfloat16):
    result = jax.random.normal(stream_key, dims, jnp.float32) * deviation
    if len(cuts) > 0:
        result = block_levels(stream_key, dims, cuts, -0.22, 0.18) * result
    return jnp.clip(result, min=-most, max=most).astype(kind)


def setup_inputs(seed: int = 0) -> dict:
    key_list = jax.random.split(jax.random.key(seed), 5)
    local_params = draw_local_params(jax.random.fold_in(key_list[4], 71), 0)
    snapshot = draw_snapshot(jax.random.fold_in(key_list[4], 71), 0)
    master = scatter_about(key_list[2], (GROUPS, ROWS, D), 1.0, 6.0, ((0, 2), (1, 128)), jnp.float32)
    momentum = scatter_about(key_list[3], (GROUPS, ROWS, D), 0.5, 4.0, ((0, 2), (1, 128)), jnp.float32)
    return dict(local_params=local_params, snapshot=snapshot, master=master, momentum=momentum)


nesterov_mu = 0.9
outer_rate = 0.7
clip_limit = 0.15
epsilon = 1e-06

def reference(local_params, snapshot, master, momentum):

    def add_replica(carry, replica):
        return (carry + replica.astype(jnp.float32), None)
    replica_sum, unused = lax.scan(add_replica, jnp.zeros(snapshot.shape, jnp.float32), local_params)
    outer_grad = snapshot.astype(jnp.float32) - replica_sum / REPLICAS
    grad_rms = jnp.sqrt(jnp.sum(outer_grad * outer_grad) / (GROUPS * ROWS * D) + epsilon)
    clipped = jnp.minimum(1.0, clip_limit / grad_rms) * outer_grad
    new_momentum = nesterov_mu * momentum + clipped
    new_master = master - outer_rate * (clipped + nesterov_mu * new_momentum)
    return (new_master, new_momentum, new_master.astype(jnp.bfloat16))
```

```python
import functools

import jax
import jax.numpy as jnp
from jax import lax
from jax.experimental import pallas as pl
from jax.experimental.pallas import tpu as pltpu
from jax.sharding import Mesh
from jax.sharding import PartitionSpec as P

REP = ("xh", "z", "y", "c")
ALL = ("xh", "z", "y", "c", "g")

nesterov_mu = 0.9
outer_rate = 0.7
clip_limit = 0.15
epsilon = 1e-06

SCALE = 32.0


def shift(axis, by):
    n = lax.axis_size(axis)
    return [(i, (i + by) % n) for i in range(n)]


def to_blocks_kernel(at, own, other, start, *outs):
    n = len(outs)
    rows, cols = own.shape
    per = rows // n
    mine = at[1]
    o = lax.broadcasted_iota(jnp.int32, (rows, rows), 0)
    r = lax.broadcasted_iota(jnp.int32, (rows, rows), 1)
    b, q = (o % per) // 4, o % 4
    dest = (o // per + mine) % n
    hit = r == b * (4 * n) + dest * 4 + q
    one = jnp.where(hit, -SCALE, 0.0).astype(jnp.bfloat16)
    two = jnp.where(hit, 2 * SCALE, 0.0).astype(jnp.bfloat16)
    dot = functools.partial(jnp.dot, preferred_element_type=jnp.float32)
    s = dot(two, start[...]) + (dot(one, own[...]) + dot(one, other[...]))
    for j, out in enumerate(outs):
        out[...] = s[j * per : (j + 1) * per].astype(out.dtype)


def to_blocks(at, own, other, start, n, wire, width=512):
    rows, half = other.shape
    steps = half // width
    mine = pl.BlockSpec((rows, width), lambda k, at: (0, at[0] * steps + k))
    plain = pl.BlockSpec((rows, width), lambda k, at: (0, k))
    return pl.pallas_call(
        to_blocks_kernel,
        grid_spec=pltpu.PrefetchScalarGridSpec(
            num_scalar_prefetch=1,
            grid=(steps,),
            in_specs=[mine, plain, mine],
            out_specs=[pl.BlockSpec((rows // n, width), lambda k, at: (0, k))] * n,
        ),
        out_shape=[jax.ShapeDtypeStruct((rows // n, half), wire)] * n,
        name="to_blocks",
    )(at, own, other, start)


def from_blocks_kernel(at, *refs):
    *ins, out = refs
    n = len(ins) // 2
    per = ins[0].shape[0]
    rows = n * per
    mine = at[1]
    r = lax.broadcasted_iota(jnp.int32, (rows, rows), 0)
    o = lax.broadcasted_iota(jnp.int32, (rows, rows), 1)
    b, q = (o % per) // 4, o % 4
    src = (mine - o // per + n) % n
    one = jnp.where(r == b * (4 * n) + src * 4 + q, 1.0, 0.0).astype(jnp.bfloat16)

    def place(blocks):
        x = jnp.concatenate([ref[...] for ref in blocks], axis=0)
        out[...] = jnp.dot(one, x, preferred_element_type=jnp.float32).astype(out.dtype)

    @pl.when(pl.program_id(0) == 0)
    def _():
        place(ins[:n])

    @pl.when(pl.program_id(0) == 1)
    def _():
        place(ins[n:])


def from_blocks(at, mine, others, width=512):
    n = len(mine)
    per, half = mine[0].shape
    steps = half // width
    first = pl.BlockSpec((per, width), lambda h, k, at: (0, jnp.where(h == 0, k, steps - 1)))
    second = pl.BlockSpec((per, width), lambda h, k, at: (0, jnp.where(h == 0, 0, k)))
    out = pl.BlockSpec((n * per, width), lambda h, k, at: (0, ((at[0] + h) % 2) * steps + k))
    return pl.pallas_call(
        from_blocks_kernel,
        grid_spec=pltpu.PrefetchScalarGridSpec(
            num_scalar_prefetch=1,
            grid=(2, steps),
            in_specs=[first] * n + [second] * n,
            out_specs=out,
        ),
        out_shape=jax.ShapeDtypeStruct((n * per, 2 * half), mine[0].dtype),
        name="from_blocks",
    )(at, *mine, *others)


def body(local_params, snapshot, master, momentum):
    replicas = lax.axis_size(REP)
    core, ys = lax.axis_index("c"), lax.axis_size("y")
    at = jnp.stack([core, lax.axis_index("y")]).astype(jnp.int32)
    local, start = local_params[0, 0], snapshot[0]
    rows, cols = local.shape
    half = cols // 2
    swap = shift("c", 1)

    send = lax.dynamic_slice(local, (0, (1 - core) * half), (rows, half))
    other = lax.ppermute(send, "c", swap)
    blocks = to_blocks(at, local, other, start, ys, jnp.float32)
    arrived = [lax.ppermute(blocks[j].astype(jnp.float16), "y", shift("y", j)) for j in (2, 1, 3)]
    total = blocks[0]
    for x in arrived:
        total = total + x.astype(jnp.float32)
    near = total.astype(jnp.float16).reshape(-1, 2, half)
    own = lax.all_to_all(near, ("xh", "z", "c"), 0, 0, tiled=True)
    summed = own.reshape(-1, 2, 2, half).astype(jnp.float32).sum(axis=0)
    outer_grad = jnp.swapaxes(summed, 0, 1).reshape(1, 2, cols) * (1.0 / (SCALE * replicas))

    part = jnp.sum(outer_grad * outer_grad)
    members = lax.axis_size(ALL)
    parts = lax.all_to_all(jnp.full((members, 1, 128), part), ALL, 0, 0, tiled=True)
    squares = jnp.sum(parts[:, 0, 0])
    elements = rows * cols * lax.axis_size("g")
    grad_rms = jnp.sqrt(squares / elements + epsilon)
    clipped = jnp.minimum(1.0, clip_limit / grad_rms) * outer_grad
    new_momentum = nesterov_mu * momentum + clipped
    new_master = master - outer_rate * (clipped + nesterov_mu * new_momentum)

    new_rows = jnp.swapaxes(new_master[0].astype(jnp.bfloat16).reshape(2, 2, half), 0, 1)
    sent = jnp.broadcast_to(new_rows[None], (near.shape[0] // 2, 2, 2, half)).reshape(near.shape)
    mine = lax.all_to_all(sent, ("xh", "z", "c"), 0, 0, tiled=True).reshape(-1, half)
    got = {j: lax.ppermute(mine, "y", shift("y", j)) for j in (2, 1, 3)}
    got[0] = mine
    got = [got[j] for j in range(ys)]
    theirs = [lax.ppermute(x, "c", swap) for x in got]
    new_params = from_blocks(at, got, theirs)
    return (new_master, new_momentum, new_params[None])


def solution(mesh):
    finer = Mesh(mesh.devices.reshape(2, 8, 4, 2, mesh.shape["grp"]), ALL)
    in_specs = (
        P(REP, "g", None, None),
        P("g", None, None),
        P("g", REP, None),
        P("g", REP, None),
    )
    out_specs = (P("g", REP, None), P("g", REP, None), P("g", None, None))
    return jax.shard_map(body, mesh=finer, in_specs=in_specs, out_specs=out_specs, check_vma=False)
```

```python
import jax
import jax.numpy as jnp
from jax import lax
from jax.experimental import pallas as pl
from jax.experimental.pallas import tpu as pltpu
from jax.sharding import Mesh
from jax.sharding import PartitionSpec as P


REP = ("xh", "z", "y", "c")
ALL = ("xh", "z", "y", "c", "g")

nesterov_mu = 0.9
outer_rate = 0.7
clip_limit = 0.15
epsilon = 1e-06

SCALE = 32.0
LAST = 4.0


def shift(axis, by):
    n = lax.axis_size(axis)
    return [(i, (i + by) % n) for i in range(n)]


def row_of(order, sign):
    ny, nz, nx = (lax.axis_size(a) for a in ("y", "z", "xh"))
    q = order % 4
    xh = order // 4 % nx
    k = order // (4 * nx) % nz
    j = order // (4 * nx * nz)
    zd = (lax.axis_index("z") + sign * k) % nz
    yd = (lax.axis_index("y") + sign * j) % ny
    return ((xh * nz + zd) * ny + yd) * 4 + q


def to_blocks_kernel(core, one, own, other, start, *outs):
    per = outs[0].shape[0]

    def placed(x):
        return jnp.dot(one[...], x[...], preferred_element_type=jnp.float32)

    s = 2.0 * placed(start) - (placed(own) + placed(other))
    for j, out in enumerate(outs):
        out[...] = s[j * per : (j + 1) * per]


def to_blocks(core, one, own, other, start, n, width=512):
    rows, half = other.shape
    steps = half // width
    mine = pl.BlockSpec((rows, width), lambda k, core: (0, core[0] * steps + k))
    plain = pl.BlockSpec((rows, width), lambda k, core: (0, k))
    return pl.pallas_call(
        to_blocks_kernel,
        grid_spec=pltpu.PrefetchScalarGridSpec(
            num_scalar_prefetch=1,
            grid=(steps,),
            in_specs=[pl.BlockSpec((rows, rows), lambda k, core: (0, 0)), mine, plain, mine],
            out_specs=[pl.BlockSpec((rows // n, width), lambda k, core: (0, k))] * n,
        ),
        out_shape=[jax.ShapeDtypeStruct((rows // n, half), jnp.float32)] * n,
        name="to_blocks",
    )(core, one, own, other, start)


def from_blocks_kernel(core, one, *refs):
    *ins, out = refs
    n = len(ins) // 2

    def place(blocks):
        x = jnp.concatenate([ref[...] for ref in blocks], axis=0)
        out[...] = jnp.dot(one[...], x, preferred_element_type=jnp.float32).astype(out.dtype)

    @pl.when(pl.program_id(0) == 0)
    def _():
        place(ins[:n])

    @pl.when(pl.program_id(0) == 1)
    def _():
        place(ins[n:])


def from_blocks(core, one, mine, others, width=1024):
    n = len(mine)
    per, half = mine[0].shape
    steps = half // width
    whole = pl.BlockSpec((n * per, n * per), lambda h, k, core: (0, 0))
    first = pl.BlockSpec((per, width), lambda h, k, core: (0, jnp.where(h == 0, k, steps - 1)))
    second = pl.BlockSpec((per, width), lambda h, k, core: (0, jnp.where(h == 0, 0, k)))
    out = pl.BlockSpec((n * per, width), lambda h, k, core: (0, ((core[0] + h) % 2) * steps + k))
    return pl.pallas_call(
        from_blocks_kernel,
        grid_spec=pltpu.PrefetchScalarGridSpec(
            num_scalar_prefetch=1,
            grid=(2, steps),
            in_specs=[whole] + [first] * n + [second] * n,
            out_specs=out,
        ),
        out_shape=jax.ShapeDtypeStruct((n * per, 2 * half), mine[0].dtype),
        name="from_blocks",
    )(core, one, *mine, *others)


def body(local_params, snapshot, master, momentum):
    replicas, ny, nz = lax.axis_size(REP), lax.axis_size("y"), lax.axis_size("z")
    core, xh = lax.axis_index("c"), lax.axis_index("xh")
    core1 = core.astype(jnp.int32)[None]
    local, start = local_params[0, 0], snapshot[0]
    rows, cols = local.shape
    half = cols // 2
    swap = shift("c", 1)
    far_y, far_z = (2, 1, 3), (4, 3, 5, 2, 6, 1, 7)

    def halves(x):
        return (lax.dynamic_slice(x, (0, s * half), (x.shape[0], half)) for s in (core, 1 - core))

    def in_order(index, x, y):
        return jnp.concatenate(
            [jnp.where(index == 0, x, y), jnp.where(index == 0, y, x)], axis=0
        )

    send = lax.dynamic_slice(local, (0, (1 - core) * half), (rows, half))
    other = lax.ppermute(send, "c", swap)
    order = jnp.arange(rows)
    to = (row_of(order, 1)[:, None] == order[None]).astype(jnp.bfloat16)
    back = (order[:, None] == row_of(order, -1)[None]).astype(jnp.bfloat16)
    blocks = to_blocks(core1, to * jnp.bfloat16(SCALE), local, other, start, ny)
    sent = {j: blocks[j].astype(jnp.float16) for j in far_y}
    total = blocks[0]
    for j in far_y:
        total = total + lax.ppermute(sent[j], "y", shift("y", j)).astype(jnp.float32)

    base, _ = lax.optimization_barrier((master[0] - outer_rate * nesterov_mu**2 * momentum[0], sent[3]))
    mine, theirs = halves(base)
    base = in_order(core, mine, lax.ppermute(theirs, "c", swap))
    base = in_order(xh, base, lax.ppermute(base, "xh", shift("xh", 1)))

    total, base = lax.optimization_barrier((total, base))
    per = rows // (ny * nz)
    pieces = [total[k * per : (k + 1) * per] for k in range(nz)]
    total = pieces[0]
    for k in far_z:
        piece = lax.ppermute(pieces[k].astype(jnp.float16), "z", shift("z", k))
        total = total + piece.astype(jnp.float32)
    total = total * (LAST / SCALE)
    total = total + lax.ppermute(total.astype(jnp.float16), "xh", shift("xh", 1)).astype(jnp.float32)
    grad = total * (1.0 / (LAST * replicas))
    grad_other = lax.ppermute(grad, "c", swap)

    part = jnp.sum(grad * grad + grad_other * grad_other)
    group = ("z", "y", "g")
    members = lax.axis_size(group)
    parts = lax.all_to_all(jnp.full((members, 1, 128), part), group, 0, 0, tiled=True)
    squares = jnp.sum(parts[:, 0, 0])
    elements = rows * cols * lax.axis_size("g")
    grad_rms = jnp.sqrt(squares / elements + epsilon)
    clip = jnp.minimum(1.0, clip_limit / grad_rms)

    new_rows = base - outer_rate * (1.0 + nesterov_mu) * (clip * grad)
    new_rows = new_rows.astype(jnp.bfloat16)
    gathered = [new_rows] + [None] * (nz - 1)
    for k in far_z:
        gathered[k] = lax.ppermute(new_rows, "z", shift("z", k))
    mine = jnp.concatenate(gathered, axis=0)
    got = [mine] + [None] * (ny - 1)
    for j in far_y:
        got[j] = lax.ppermute(mine, "y", shift("y", j))
    theirs = [lax.ppermute(x, "c", swap) for x in got]
    new_params = from_blocks(core1, back, got, theirs)

    at = (xh * 2 + core) * 2
    own = [lax.dynamic_slice(x, (at, 0), (2, half)) for x in (grad, grad_other)]
    low, high = jnp.where(core == 0, own[0], own[1]), jnp.where(core == 0, own[1], own[0])
    clipped = clip * jnp.concatenate([low, high], axis=1)[None]
    new_momentum = nesterov_mu * momentum + clipped
    new_master = master - outer_rate * (clipped + nesterov_mu * new_momentum)
    return (new_master, new_momentum, new_params[None])


def solution(mesh):
    finer = Mesh(mesh.devices.reshape(2, 8, 4, 2, mesh.shape["grp"]), ALL)
    in_specs = (
        P(REP, "g", None, None),
        P("g", None, None),
        P("g", REP, None),
        P("g", REP, None),
    )
    out_specs = (P("g", REP, None), P("g", REP, None), P("g", None, None))
    return jax.shard_map(body, mesh=finer, in_specs=in_specs, out_specs=out_specs, check_vma=False)
```

```python
import jax
import jax.numpy as jnp
from jax import lax
from jax.experimental import pallas as pl
from jax.experimental.pallas import tpu as pltpu
from jax.sharding import Mesh
from jax.sharding import PartitionSpec as P


REP = ("xh", "z", "y", "c")
ALL = ("xh", "z", "y", "c", "g")

nesterov_mu = 0.9
outer_rate = 0.7
clip_limit = 0.15
epsilon = 1e-06

SCALE = 16.0
WIDTH = 1024
MIB = 1024 * 1024
VMEM = pl.BlockSpec(memory_space=pltpu.VMEM)


def shift(axis, by):
    n = lax.axis_size(axis)
    return [(i, (i + by) % n) for i in range(n)]


def row_of(j, h, z, q, sign):
    ny, nz, nx = (lax.axis_size(a) for a in ("y", "z", "xh"))
    yd = (lax.axis_index("y") + sign * j) % ny
    xd = (lax.axis_index("xh") + h) % nx
    return ((xd * nz + z) * ny + yd) * 4 + q


def change_kernel(core, one, own, start, out):
    placed = [jnp.dot(one[...], x[...], preferred_element_type=jnp.float32) for x in (start, own)]
    out[...] = 2.0 * placed[0] - placed[1]


def change(core, one, own, start):
    rows, cols = own.shape
    steps = cols // 2 // WIDTH
    mine = pl.BlockSpec((rows, WIDTH), lambda k, core: (0, core[0] * steps + k))
    return pl.pallas_call(
        change_kernel,
        grid_spec=pltpu.PrefetchScalarGridSpec(
            num_scalar_prefetch=1,
            grid=(steps,),
            in_specs=[pl.BlockSpec((rows, rows), lambda k, core: (0, 0)), mine, mine],
            out_specs=pl.BlockSpec((rows, WIDTH), lambda k, core: (0, k)),
        ),
        out_shape=jax.ShapeDtypeStruct((rows, cols // 2), jnp.float32),
        compiler_params=pltpu.CompilerParams(vmem_limit_bytes=10 * MIB),
        name="change",
    )(core, one, own, start)


def to_blocks_kernel(one, own, other, *outs):
    *by_y, near, far = outs
    half, per = other.shape[1], by_y[0].shape[0]
    edge = by_y[0].shape[1]
    for at in range(0, half, WIDTH):
        here = slice(at, at + WIDTH)
        s = own[:, here] - jnp.dot(one[...], other[:, here], preferred_element_type=jnp.float32)
        for j in range(len(by_y)):
            block = s[j * per : (j + 1) * per]
            if at < edge:
                by_y[j][:, here] = block
            else:
                to = slice(j * per // 2, (j + 1) * per // 2), slice(at - edge, at - edge + WIDTH)
                near[to] = block[: per // 2]
                far[to] = block[per // 2 :]


def to_blocks(one, own, other, n):
    rows, half = other.shape
    shapes = [(rows // n, half // 2)] * n + [(rows // 2, half // 2)] * 2
    return pl.pallas_call(
        to_blocks_kernel,
        in_specs=[VMEM, VMEM, VMEM],
        out_specs=[VMEM] * len(shapes),
        out_shape=[jax.ShapeDtypeStruct(s, jnp.float32) for s in shapes],
        compiler_params=pltpu.CompilerParams(vmem_limit_bytes=6 * MIB),
        name="to_blocks",
    )(one, own, other)


def from_blocks_kernel(core, first, second, *refs):
    *ins, out = refs
    n = len(ins) // 2
    parts = ins[0].shape[1] // WIDTH
    side, k = pl.program_id(0), pl.program_id(1)

    def place(one, blocks, part):
        x = jnp.concatenate([b[:, part * WIDTH : (part + 1) * WIDTH] for b in blocks], axis=0)
        out[...] = jnp.dot(one[...], x, preferred_element_type=jnp.float32).astype(out.dtype)

    for s in range(2):
        mine = ins[s * n : (s + 1) * n]
        for part in range(parts):

            @pl.when((side == s) & (k == part))
            def _():
                place(first, mine[:-2], part)

            @pl.when((side == s) & (k == parts + part))
            def _():
                place(second, mine[-2:], part)


def from_blocks(core, first, second, mine, theirs):
    rows, width = first.shape[0], 4 * mine[0].shape[1]
    steps = width // 2 // WIDTH
    whole = pl.BlockSpec(memory_space=pltpu.VMEM)
    return pl.pallas_call(
        from_blocks_kernel,
        grid_spec=pltpu.PrefetchScalarGridSpec(
            num_scalar_prefetch=1,
            grid=(2, steps),
            in_specs=[whole] * (2 + len(mine) + len(theirs)),
            out_specs=pl.BlockSpec((rows, WIDTH), lambda s, k, core: (0, (core[0] + s) % 2 * steps + k)),
        ),
        out_shape=jax.ShapeDtypeStruct((rows, width), mine[0].dtype),
        compiler_params=pltpu.CompilerParams(vmem_limit_bytes=10 * MIB),
        name="from_blocks",
    )(core, first, second, *mine, *theirs)


def body(local_params, snapshot, master, momentum):
    replicas, ny, nz, nx = (lax.axis_size(a) for a in (REP, "y", "z", "xh"))
    core = lax.axis_index("c")
    core1 = core.astype(jnp.int32)[None]
    local, start = local_params[0, 0], snapshot[0]
    rows, cols = local.shape
    half = cols // 2
    edge = half // 2
    far_y = (2, 1, 3)
    wire = jnp.float16

    def to_core(x):
        return lax.ppermute(x, "c", shift("c", 1))

    def to_x(x):
        return lax.ppermute(x, "xh", shift("xh", 1))

    def to_y(x, j):
        return lax.ppermute(x, "y", shift("y", j))

    def wide(x):
        return x.astype(jnp.float32)

    other = to_core(lax.dynamic_slice(local, (0, (1 - core) * half), (rows, half)))
    o = jnp.arange(rows)
    q, z, h, j = o % 4, o // 4 % nz, o // (4 * nz) % nx, o // (4 * nz * nx)
    to = row_of(j, h, z, q, 1)[:, None] == o[None]
    back_y = o[:, None] == row_of(j, h, z, q, -1)[None]
    j, h = o // (4 * nz) % ny, o // (4 * nz * ny)
    back_x = o[:, None] == row_of(j, h, z, q, -1)[None]

    to = jnp.where(to, SCALE, 0.0).astype(jnp.bfloat16)
    *by_y, near, far = to_blocks(to, change(core1, to, local, start), other, ny)
    far = far.astype(wire)
    by_y = [by_y[0]] + [x.astype(wire) for x in by_y[1:]]
    first, second = by_y[0], near
    second = second + wide(to_x(far))
    for j in far_y:
        first = first + wide(to_y(by_y[j], j))
    per = rows // (nx * ny)
    base, _ = lax.optimization_barrier((master[0] - outer_rate * nesterov_mu**2 * momentum[0], first))
    mine, theirs = (lax.dynamic_slice(base, (0, s * half), (2, half)) for s in (core, 1 - core))
    theirs = to_core(theirs)
    base = jnp.concatenate([jnp.where(core == 0, mine, theirs), jnp.where(core == 0, theirs, mine)], axis=0)
    pieces = [second[j * per : (j + 1) * per] for j in range(ny)]
    second = pieces[0]
    far = to_x(first[per:].astype(wire))
    for j in far_y:
        second = second + wide(to_y(pieces[j].astype(wire), j))
    first = first[:per] + wide(far)

    total = jnp.concatenate([first, second], axis=1).astype(wire).reshape(nz, 4, half)
    base, total = lax.optimization_barrier((base, total))
    total = wide(lax.all_to_all(total, "z", 0, 0, tiled=True)).sum(axis=0)
    grad = total * (1.0 / (SCALE * replicas))
    grad_other = to_core(lax.dynamic_slice(grad, (2 * (1 - core), 0), (2, half)))

    members = lax.axis_size(ALL)
    parts = lax.all_to_all(jnp.full((members, 1, 128), jnp.sum(grad * grad)), ALL, 0, 0, tiled=True)
    squares = jnp.sum(parts[:, 0, 0])
    elements = rows * cols * lax.axis_size("g")
    grad_rms = jnp.sqrt(squares / elements + epsilon)
    clip = jnp.minimum(1.0, clip_limit / grad_rms)

    new_rows = (base - outer_rate * (1.0 + nesterov_mu) * (clip * grad)).astype(jnp.bfloat16)
    mine = lax.all_to_all(jnp.broadcast_to(new_rows[None], (nz, 4, half)), "z", 0, 0, tiled=True)
    mine = mine.reshape(nz * 4, half)
    first, second = mine[:, :edge], mine[:, edge:]
    first = jnp.concatenate([first, to_x(first)], axis=0)
    arrived = {j: to_y(second, j) for j in far_y}
    second = jnp.concatenate([second] + [arrived[j] for j in range(1, ny)], axis=0)
    arrived = {j: to_y(first, j) for j in far_y}
    mine = [first] + [arrived[j] for j in range(1, ny)] + [second, to_x(second)]
    theirs = [to_core(x) for x in mine]
    new_params = from_blocks(core1, back_y.astype(jnp.bfloat16), back_x.astype(jnp.bfloat16), mine, theirs)

    own = lax.dynamic_slice(grad, (2 * core, 0), (2, half))
    own = [jnp.where(core == 0, own, grad_other), jnp.where(core == 0, grad_other, own)]
    clipped = clip * jnp.concatenate(own, axis=1)[None]
    new_momentum = nesterov_mu * momentum + clipped
    new_master = master - outer_rate * (clipped + nesterov_mu * new_momentum)
    return (new_master, new_momentum, new_params[None])


def solution(mesh):
    finer = Mesh(mesh.devices.reshape(2, 8, 4, 2, mesh.shape["grp"]), ALL)
    in_specs = (
        P(REP, "g", None, None),
        P("g", None, None),
        P("g", REP, None),
        P("g", REP, None),
    )
    out_specs = (P("g", REP, None), P("g", REP, None), P("g", None, None))
    return jax.shard_map(body, mesh=finer, in_specs=in_specs, out_specs=out_specs, check_vma=False)
```

```python
import jax
import jax.numpy as jnp
from jax import lax
from jax.experimental import pallas as pl
from jax.experimental.pallas import tpu as pltpu
from jax.sharding import Mesh
from jax.sharding import PartitionSpec as P


REP = ("xh", "z", "y", "c")
ALL = ("xh", "z", "y", "c", "g")

nesterov_mu = 0.9
outer_rate = 0.7
clip_limit = 0.15
epsilon = 1e-06

SCALE = 16.0
WIDTH = 1024
MIB = 1024 * 1024
VMEM = pl.BlockSpec(memory_space=pltpu.VMEM)
SMEM = pl.BlockSpec(memory_space=pltpu.SMEM)
HBM = pl.BlockSpec(memory_space=pltpu.HBM)


def shift(axis, by):
    n = lax.axis_size(axis)
    return [(i, (i + by) % n) for i in range(n)]


def row_of(j, h, z, q, sign):
    ny, nz, nx = (lax.axis_size(a) for a in ("y", "z", "xh"))
    yd = (lax.axis_index("y") + sign * j) % ny
    xd = (lax.axis_index("xh") + h) % nx
    return ((xd * nz + z) * ny + yd) * 4 + q


def pick_kernel(core, local, out, sem):
    half = out.shape[1]
    begin = pl.multiple_of((1 - core[0]) * half, half)
    copy = pltpu.make_async_copy(local.at[:, pl.ds(begin, half)], out, sem)
    copy.start()
    copy.wait()


def pick(core, local):
    rows, cols = local.shape
    return pl.pallas_call(
        pick_kernel,
        in_specs=[SMEM, HBM],
        out_specs=VMEM,
        out_shape=jax.ShapeDtypeStruct((rows, cols // 2), local.dtype),
        scratch_shapes=[pltpu.SemaphoreType.DMA],
        compiler_params=pltpu.CompilerParams(vmem_limit_bytes=61 * MIB),
        name="pick",
    )(core, local)


def change_kernel(core, one, own, start, out, held, sems):
    _, half = out.shape
    copies = []
    for k in range(half // WIDTH):
        begin = pl.multiple_of(core[0] * half + k * WIDTH, WIDTH)
        for i, x in enumerate((own, start)):
            to = held.at[i, :, pl.ds(k * WIDTH, WIDTH)]
            copies.append(pltpu.make_async_copy(x.at[:, pl.ds(begin, WIDTH)], to, sems.at[i, k]))
    for copy in copies:
        copy.start()
    for k in range(half // WIDTH):
        copies[2 * k].wait()
        copies[2 * k + 1].wait()
        here = slice(k * WIDTH, (k + 1) * WIDTH)
        placed = [jnp.dot(one[...], held[i, :, here], preferred_element_type=jnp.float32) for i in range(2)]
        out[:, here] = 2.0 * placed[1] - placed[0]


def change(core, one, own, start):
    rows, cols = own.shape
    half = cols // 2
    return pl.pallas_call(
        change_kernel,
        in_specs=[SMEM, VMEM, HBM, HBM],
        out_specs=VMEM,
        out_shape=jax.ShapeDtypeStruct((rows, half), jnp.float32),
        scratch_shapes=[
            pltpu.VMEM((2, rows, half), own.dtype),
            pltpu.SemaphoreType.DMA((2, half // WIDTH)),
        ],
        compiler_params=pltpu.CompilerParams(vmem_limit_bytes=52 * MIB),
        name="change",
    )(core, one, own, start)


def to_blocks_kernel(one, own, other, *outs):
    *by_y, near, far = outs
    half, per = other.shape[1], by_y[0].shape[0]
    edge = by_y[0].shape[1]
    for at in range(0, half, WIDTH):
        here = slice(at, at + WIDTH)
        s = own[:, here] - jnp.dot(one[...], other[:, here], preferred_element_type=jnp.float32)
        for j in range(len(by_y)):
            block = s[j * per : (j + 1) * per]
            if at < edge:
                by_y[j][:, here] = block
            else:
                to = slice(j * per // 2, (j + 1) * per // 2), slice(at - edge, at - edge + WIDTH)
                near[to] = block[: per // 2]
                far[to] = block[per // 2 :]


def to_blocks(one, own, other, n):
    rows, half = other.shape
    shapes = [(rows // n, half // 2)] * n + [(rows // 2, half // 2)] * 2
    return pl.pallas_call(
        to_blocks_kernel,
        in_specs=[VMEM, VMEM, VMEM],
        out_specs=[VMEM] * len(shapes),
        out_shape=[jax.ShapeDtypeStruct(s, jnp.float32) for s in shapes],
        compiler_params=pltpu.CompilerParams(vmem_limit_bytes=6 * MIB),
        name="to_blocks",
    )(one, own, other)


def from_blocks_kernel(core, first, second, *refs):
    *ins, out = refs
    n = len(ins) // 2
    parts = ins[0].shape[1] // WIDTH
    side, k = pl.program_id(0), pl.program_id(1)

    def place(one, blocks, part):
        x = jnp.concatenate([b[:, part * WIDTH : (part + 1) * WIDTH] for b in blocks], axis=0)
        out[...] = jnp.dot(one[...], x, preferred_element_type=jnp.float32).astype(out.dtype)

    for s in range(2):
        mine = ins[s * n : (s + 1) * n]
        for part in range(parts):

            @pl.when((side == s) & (k == part))
            def _():
                place(first, mine[:-2], part)

            @pl.when((side == s) & (k == parts + part))
            def _():
                place(second, mine[-2:], part)


def from_blocks(core, first, second, mine, theirs):
    rows, width = first.shape[0], 4 * mine[0].shape[1]
    steps = width // 2 // WIDTH
    whole = pl.BlockSpec(memory_space=pltpu.VMEM)
    return pl.pallas_call(
        from_blocks_kernel,
        grid_spec=pltpu.PrefetchScalarGridSpec(
            num_scalar_prefetch=1,
            grid=(2, steps),
            in_specs=[whole] * (2 + len(mine) + len(theirs)),
            out_specs=pl.BlockSpec((rows, WIDTH), lambda s, k, core: (0, (core[0] + s) % 2 * steps + k)),
        ),
        out_shape=jax.ShapeDtypeStruct((rows, width), mine[0].dtype),
        compiler_params=pltpu.CompilerParams(vmem_limit_bytes=10 * MIB),
        name="from_blocks",
    )(core, first, second, *mine, *theirs)


def step(local_params, snapshot, master, momentum):
    replicas, ny, nz, nx = (lax.axis_size(a) for a in (REP, "y", "z", "xh"))
    core = lax.axis_index("c")
    core1 = core.astype(jnp.int32)[None]
    local, start = local_params[0, 0], snapshot[0]
    rows, cols = local.shape
    half = cols // 2
    edge = half // 2
    far_y = (2, 1, 3)
    wire = jnp.float16

    def send(x, axis, by):
        return lax.ppermute(x, axis, shift(axis, by))

    def wide(x):
        return x.astype(jnp.float32)

    other = send(pick(core1, local), "c", 1)
    o = jnp.arange(rows)
    q, z, h, j = o % 4, o // 4 % nz, o // (4 * nz) % nx, o // (4 * nz * nx)
    to = row_of(j, h, z, q, 1)[:, None] == o[None]
    z = (lax.axis_index("z") - z) % nz
    back_y = o[:, None] == row_of(j, h, z, q, -1)[None]
    j, h = o // (4 * nz) % ny, o // (4 * nz * ny)
    back_x = o[:, None] == row_of(j, h, z, q, -1)[None]

    to = jnp.where(to, SCALE, 0.0).astype(jnp.bfloat16)
    *by_y, near, far = to_blocks(to, change(core1, to, local, start), other, ny)
    far = far.astype(wire)
    by_y = [by_y[0]] + [x.astype(wire) for x in by_y[1:]]
    first, second = by_y[0], near
    second = second + wide(send(far, "xh", 1))
    for j in far_y:
        first = first + wide(send(by_y[j], "y", j))

    old, _ = lax.optimization_barrier(((master, momentum), (far, by_y[1:])))
    base = old[0][0] - outer_rate * nesterov_mu**2 * old[1][0]
    mine, theirs = (lax.dynamic_slice(base, (0, s * half), (2, half)) for s in (core, 1 - core))
    theirs = send(theirs, "c", 1)
    base = jnp.concatenate([jnp.where(core == 0, mine, theirs), jnp.where(core == 0, theirs, mine)], axis=0)
    base = lax.all_to_all(jnp.broadcast_to(base[None], (nz, 4, half)), "z", 0, 0, tiled=True)

    per = rows // (nx * ny)
    pieces = [second[j * per : (j + 1) * per] for j in range(ny)]
    second = pieces[0]
    far = send(first[per:].astype(wire), "xh", 1)
    for j in far_y:
        second = second + wide(send(pieces[j].astype(wire), "y", j))
    first = first[:per] + wide(far)

    total = jnp.concatenate([first, second], axis=1).astype(wire).reshape(nz, 4, half)
    base, total = lax.optimization_barrier((base, total))
    total = wide(lax.all_to_all(total, "z", 0, 0, tiled=True)).sum(axis=0)
    grad = total * (1.0 / (SCALE * replicas))
    grads = {k: send(grad, "z", k) for k in (4, 3, 5, 2, 6, 1, 7)}
    grads[0] = grad

    members = lax.axis_size(ALL)
    parts = lax.all_to_all(jnp.full((members, 1, 128), jnp.sum(grad * grad)), ALL, 0, 0, tiled=True)
    squares = jnp.sum(parts[:, 0, 0])
    elements = rows * cols * lax.axis_size("g")
    grad_rms = jnp.sqrt(squares / elements + epsilon)
    clip = jnp.minimum(1.0, clip_limit / grad_rms)

    mine = []
    for k in range(nz):
        there = lax.dynamic_index_in_dim(base, lax.rem(lax.axis_index("z") + (nz - k), nz), 0, keepdims=False)
        mine.append((there - outer_rate * (1.0 + nesterov_mu) * (clip * grads[k])).astype(jnp.bfloat16))
    mine = jnp.concatenate(mine, axis=0)
    first, second = mine[:, :edge], mine[:, edge:]
    arrived = {j: send(second, "y", j) for j in far_y}
    second = jnp.concatenate([second] + [arrived[j] for j in range(1, ny)], axis=0)
    first = jnp.concatenate([first, send(first, "xh", 1)], axis=0)
    arrived = {j: send(first, "y", j) for j in far_y}
    mine = [first] + [arrived[j] for j in range(1, ny)] + [second, send(second, "xh", 1)]
    theirs = [send(x, "c", 1) for x in mine]
    new_params = from_blocks(core1, back_y.astype(jnp.bfloat16), back_x.astype(jnp.bfloat16), mine, theirs)

    other = send(lax.dynamic_slice(grad, (2 * (1 - core), 0), (2, half)), "c", 1)
    own = lax.dynamic_slice(grad, (2 * core, 0), (2, half))
    own = [jnp.where(core == 0, own, other), jnp.where(core == 0, other, own)]
    clipped = clip * jnp.concatenate(own, axis=1)[None]
    new_momentum = nesterov_mu * momentum + clipped
    new_master = master - outer_rate * (clipped + nesterov_mu * new_momentum)
    return (new_master, new_momentum, new_params[None])


def solution(mesh):
    finer = Mesh(mesh.devices.reshape(2, 8, 4, 2, mesh.shape["grp"]), ALL)
    in_specs = (
        P(REP, "g", None, None),
        P("g", None, None),
        P("g", REP, None),
        P("g", REP, None),
    )
    out_specs = (P("g", REP, None), P("g", REP, None), P("g", None, None))
    return jax.shard_map(step, mesh=finer, in_specs=in_specs, out_specs=out_specs, check_vma=False)
```

```python
import jax
import jax.numpy as jnp
from jax import lax
from jax.experimental import pallas as pl
from jax.experimental.pallas import tpu as pltpu
from jax.sharding import Mesh
from jax.sharding import PartitionSpec as P


REP = ("xh", "z", "y", "c")
ALL = ("xh", "z", "y", "c", "g")

nesterov_mu = 0.9
outer_rate = 0.7
clip_limit = 0.15
epsilon = 1e-06

SCALE = 16.0
WIDTH = 1024
MIB = 1024 * 1024
VMEM = pl.BlockSpec(memory_space=pltpu.VMEM)
SMEM = pl.BlockSpec(memory_space=pltpu.SMEM)
HBM = pl.BlockSpec(memory_space=pltpu.HBM)


def shift(axis, by):
    n = lax.axis_size(axis)
    return [(i, (i + by) % n) for i in range(n)]


def row_of(j, h, z, q, sign):
    ny, nz, nx = (lax.axis_size(a) for a in ("y", "z", "xh"))
    yd = (lax.axis_index("y") + sign * j) % ny
    xd = (lax.axis_index("xh") + h) % nx
    return ((xd * nz + z) * ny + yd) * 4 + q


def pick_kernel(core, local, out, sem):
    half = out.shape[1]
    begin = pl.multiple_of((1 - core[0]) * half, half)
    copy = pltpu.make_async_copy(local.at[:, pl.ds(begin, half)], out, sem)
    copy.start()
    copy.wait()


def pick(core, local):
    rows, cols = local.shape
    return pl.pallas_call(
        pick_kernel,
        in_specs=[SMEM, HBM],
        out_specs=VMEM,
        out_shape=jax.ShapeDtypeStruct((rows, cols // 2), local.dtype),
        scratch_shapes=[pltpu.SemaphoreType.DMA],
        compiler_params=pltpu.CompilerParams(vmem_limit_bytes=59 * MIB),
        name="pick",
    )(core, local)


def change_kernel(core, one, own, start, out, held, sems):
    _, half = out.shape
    copies = []
    for k in range(half // WIDTH):
        begin = pl.multiple_of(core[0] * half + k * WIDTH, WIDTH)
        for i, x in enumerate((own, start)):
            to = held.at[i, :, pl.ds(k * WIDTH, WIDTH)]
            copies.append(pltpu.make_async_copy(x.at[:, pl.ds(begin, WIDTH)], to, sems.at[i, k]))
    for copy in copies:
        copy.start()
    for k in range(half // WIDTH):
        copies[2 * k].wait()
        copies[2 * k + 1].wait()
        here = slice(k * WIDTH, (k + 1) * WIDTH)
        placed = [jnp.dot(one[...], held[i, :, here], preferred_element_type=jnp.float32) for i in range(2)]
        out[:, here] = 2.0 * placed[1] - placed[0]


def change(core, one, own, start):
    rows, cols = own.shape
    half = cols // 2
    return pl.pallas_call(
        change_kernel,
        in_specs=[SMEM, VMEM, HBM, HBM],
        out_specs=VMEM,
        out_shape=jax.ShapeDtypeStruct((rows, half), jnp.float32),
        scratch_shapes=[
            pltpu.VMEM((2, rows, half), own.dtype),
            pltpu.SemaphoreType.DMA((2, half // WIDTH)),
        ],
        compiler_params=pltpu.CompilerParams(vmem_limit_bytes=49 * MIB),
        name="change",
    )(core, one, own, start)


def to_blocks_kernel(one, own, other, *outs):
    *by_y, near, far = outs
    half, per = other.shape[1], by_y[0].shape[0]
    edge = by_y[0].shape[1]
    for at in range(0, half, WIDTH):
        here = slice(at, at + WIDTH)
        s = own[:, here] - jnp.dot(one[...], other[:, here], preferred_element_type=jnp.float32)
        for j in range(len(by_y)):
            block = s[j * per : (j + 1) * per]
            if at < edge:
                by_y[j][:, here] = block
            else:
                to = slice(j * per // 2, (j + 1) * per // 2), slice(at - edge, at - edge + WIDTH)
                near[to] = block[: per // 2]
                far[to] = block[per // 2 :]


def to_blocks(one, own, other, n):
    rows, half = other.shape
    shapes = [(rows // n, half // 2)] * n + [(rows // 2, half // 2)] * 2
    return pl.pallas_call(
        to_blocks_kernel,
        in_specs=[VMEM, VMEM, VMEM],
        out_specs=[VMEM] * len(shapes),
        out_shape=[jax.ShapeDtypeStruct(s, jnp.float32) for s in shapes],
        compiler_params=pltpu.CompilerParams(vmem_limit_bytes=6 * MIB),
        name="to_blocks",
    )(one, own, other)


def from_blocks_kernel(core, one, *refs):
    out = refs[-1]
    n = (len(refs) - 1) // 2
    ins = refs[: 2 * n]
    side, k = pl.program_id(0), pl.program_id(1)
    for s in range(2):
        for part in range(ins[0].shape[1] // WIDTH):

            @pl.when((side == s) & (k == part))
            def _():
                blocks = [b[:, part * WIDTH : (part + 1) * WIDTH] for b in ins[s * n : (s + 1) * n]]
                x = jnp.concatenate(blocks, axis=0)
                out[...] = jnp.dot(one[...], x, preferred_element_type=jnp.float32).astype(out.dtype)


def from_blocks(core, one, mine, theirs, quarter, out=None):
    rows, width = one.shape[0], 4 * mine[0].shape[1]
    steps = mine[0].shape[1] // WIDTH
    blocks = [*mine, *theirs]
    rest = [] if out is None else [out]
    return pl.pallas_call(
        from_blocks_kernel,
        grid_spec=pltpu.PrefetchScalarGridSpec(
            num_scalar_prefetch=1,
            grid=(2, steps),
            in_specs=[VMEM] * (1 + len(blocks)) + [HBM] * len(rest),
            out_specs=pl.BlockSpec(
                (rows, WIDTH), lambda s, k, core: (0, ((core[0] + s) % 2 * 2 + quarter) * steps + k)
            ),
        ),
        out_shape=jax.ShapeDtypeStruct((rows, width), mine[0].dtype),
        input_output_aliases={2 + len(blocks): 0} if rest else {},
        compiler_params=pltpu.CompilerParams(vmem_limit_bytes=10 * MIB),
        name="from_blocks",
    )(core, one, *blocks, *rest)


def step(local_params, snapshot, master, momentum):
    replicas, ny, nz, nx = (lax.axis_size(a) for a in (REP, "y", "z", "xh"))
    core = lax.axis_index("c")
    core1 = core.astype(jnp.int32)[None]
    local, start = local_params[0, 0], snapshot[0]
    rows, cols = local.shape
    half = cols // 2
    edge = half // 2
    far_y = (2, 1, 3)
    wire = jnp.float16

    def send(x, axis, by):
        return lax.ppermute(x, axis, shift(axis, by))

    def part(x, row, col):
        return lax.dynamic_slice(x, (row, col), (2, half), allow_negative_indices=False)

    def wide(x):
        return x.astype(jnp.float32)

    o = jnp.arange(rows)
    q, z, h, j = o % 4, o // 4 % nz, o // (4 * nz) % nx, o // (4 * nz * nx)
    to = row_of(j, h, z, q, 1)[:, None] == o[None]
    z = (lax.axis_index("z") - z) % nz
    back_y = o[:, None] == row_of(j, h, z, q, -1)[None]
    j, h = o // (4 * nz) % ny, o // (4 * nz * ny)
    back_x = o[:, None] == row_of(j, h, z, q, -1)[None]

    to = jnp.where(to, SCALE, 0.0).astype(jnp.bfloat16)
    at = (core * half, (1 - core) * half, 2 * core, 2 * (1 - core))
    local, start, to, at, core1 = lax.optimization_barrier((local, start, to, at, core1))
    other = send(pick(core1, local), "c", 1)
    *by_y, near, far = to_blocks(to, change(core1, to, local, start), other, ny)
    far, near = far.astype(wire), near.astype(wire)
    by_y = [x.astype(wire) for x in by_y]
    first, second = wide(by_y[0]), wide(near)
    second = second + wide(send(far, "xh", 1))
    for j in far_y:
        first = first + wide(send(by_y[j], "y", j))

    old, _ = lax.optimization_barrier(((master, momentum), (far, by_y[1:])))
    base = old[0][0] - outer_rate * nesterov_mu**2 * old[1][0]
    mine, theirs = part(base, 0, at[0]), part(base, 0, at[1])
    theirs = send(theirs, "c", 1)
    base = jnp.concatenate([jnp.where(core == 0, mine, theirs), jnp.where(core == 0, theirs, mine)], axis=0)

    per = rows // (nx * ny)
    pieces = [second[j * per : (j + 1) * per] for j in range(ny)]
    second = pieces[0]
    far = send(first[per:].astype(wire), "xh", 1)
    for j in far_y:
        second = second + wide(send(pieces[j].astype(wire), "y", j))
    first = first[:per] + wide(far)

    total = jnp.concatenate([first, second], axis=1).astype(wire).reshape(nz, 4, half)
    base, total = lax.optimization_barrier((base, total))
    total = wide(lax.all_to_all(total, "z", 0, 0, tiled=True)).sum(axis=0)
    grad = total * (1.0 / (SCALE * replicas))
    grad = lax.optimization_barrier(grad)
    pair = lax.optimization_barrier(jnp.concatenate([base, grad], axis=1))
    pairs = {k: send(pair, "z", k) for k in (4, 3, 5, 2, 6, 1, 7)}
    pairs[0] = pair

    members = lax.axis_size(ALL)
    parts = lax.all_to_all(jnp.full((members, 1, 128), jnp.sum(grad * grad)), ALL, 0, 0, tiled=True)
    squares = jnp.sum(parts[:, 0, 0])
    elements = rows * cols * lax.axis_size("g")
    grad_rms = jnp.sqrt(squares / elements + epsilon)
    clip = jnp.minimum(1.0, clip_limit / grad_rms)

    pairs = [pairs[k] for k in range(nz)]
    mine = [x[:, :half] - outer_rate * (1.0 + nesterov_mu) * (clip * x[:, half:]) for x in pairs]
    mine = [x.astype(jnp.bfloat16) for x in mine]
    mine = jnp.concatenate(mine, axis=0)
    first, second = mine[:, :edge], mine[:, edge:]
    arrived = {j: send(second, "y", j) for j in far_y}
    second = jnp.concatenate([second] + [arrived[j] for j in range(1, ny)], axis=0)
    first = jnp.concatenate([first, send(first, "xh", 1)], axis=0)
    arrived = {j: send(first, "y", j) for j in far_y}
    mine = [first] + [arrived[j] for j in range(1, ny)]
    theirs = [send(x, "c", 1) for x in mine]
    new_params = from_blocks(core1, back_y.astype(jnp.bfloat16), mine, theirs, 0)
    mine = [second, send(second, "xh", 1)]
    theirs = [send(x, "c", 1) for x in mine]
    new_params = from_blocks(core1, back_x.astype(jnp.bfloat16), mine, theirs, 1, new_params)

    other = send(part(grad, at[3], 0), "c", 1)
    own = part(grad, at[2], 0)
    own = [jnp.where(core == 0, own, other), jnp.where(core == 0, other, own)]
    clipped = clip * jnp.concatenate(own, axis=1)[None]
    new_momentum = nesterov_mu * momentum + clipped
    new_master = master - outer_rate * (clipped + nesterov_mu * new_momentum)
    return (new_master, new_momentum, new_params[None])


def solution(mesh):
    finer = Mesh(mesh.devices.reshape(2, 8, 4, 2, mesh.shape["grp"]), ALL)
    in_specs = (
        P(REP, "g", None, None),
        P("g", None, None),
        P("g", REP, None),
        P("g", REP, None),
    )
    out_specs = (P("g", REP, None), P("g", REP, None), P("g", None, None))
    return jax.shard_map(step, mesh=finer, in_specs=in_specs, out_specs=out_specs, check_vma=False)
```

```python
import jax
import jax.numpy as jnp
from jax import lax
from jax.experimental import pallas as pl
from jax.experimental.pallas import tpu as pltpu
from jax.sharding import Mesh
from jax.sharding import PartitionSpec as P


REP = ("xh", "z", "y", "c")
ALL = ("xh", "z", "y", "c", "g")

nesterov_mu = 0.9
outer_rate = 0.7
clip_limit = 0.15
epsilon = 1e-06

SCALE = 16.0
WIDTH = 1024
MIB = 1024 * 1024
VMEM = pl.BlockSpec(memory_space=pltpu.VMEM)
SMEM = pl.BlockSpec(memory_space=pltpu.SMEM)
HBM = pl.BlockSpec(memory_space=pltpu.HBM)


def shift(axis, by):
    n = lax.axis_size(axis)
    return [(i, (i + by) % n) for i in range(n)]


def row_of(j, h, z, q, sign):
    ny, nz, nx = (lax.axis_size(a) for a in ("y", "z", "xh"))
    yd = (lax.axis_index("y") + sign * j) % ny
    xd = (lax.axis_index("xh") + h) % nx
    return ((xd * nz + z) * ny + yd) * 4 + q


def pick_kernel(core, local, out, sem):
    half = out.shape[1]
    begin = pl.multiple_of((1 - core[0]) * half, half)
    copy = pltpu.make_async_copy(local.at[:, pl.ds(begin, half)], out, sem)
    copy.start()
    copy.wait()


def pick(core, local):
    rows, cols = local.shape
    return pl.pallas_call(
        pick_kernel,
        in_specs=[SMEM, HBM],
        out_specs=VMEM,
        out_shape=jax.ShapeDtypeStruct((rows, cols // 2), local.dtype),
        scratch_shapes=[pltpu.SemaphoreType.DMA],
        compiler_params=pltpu.CompilerParams(vmem_limit_bytes=59 * MIB),
        name="pick",
    )(core, local)


def change_kernel(core, one, own, start, out, held, sems):
    _, half = out.shape
    copies = []
    for k in range(half // WIDTH):
        begin = pl.multiple_of(core[0] * half + k * WIDTH, WIDTH)
        for i, x in enumerate((own, start)):
            to = held.at[i, :, pl.ds(k * WIDTH, WIDTH)]
            copies.append(pltpu.make_async_copy(x.at[:, pl.ds(begin, WIDTH)], to, sems.at[i, k]))
    for copy in copies:
        copy.start()
    for k in range(half // WIDTH):
        copies[2 * k].wait()
        copies[2 * k + 1].wait()
        here = slice(k * WIDTH, (k + 1) * WIDTH)
        placed = [jnp.dot(one[...], held[i, :, here], preferred_element_type=jnp.float32) for i in range(2)]
        out[:, here] = 2.0 * placed[1] - placed[0]


def change(core, one, own, start):
    rows, cols = own.shape
    half = cols // 2
    return pl.pallas_call(
        change_kernel,
        in_specs=[SMEM, VMEM, HBM, HBM],
        out_specs=VMEM,
        out_shape=jax.ShapeDtypeStruct((rows, half), jnp.float32),
        scratch_shapes=[
            pltpu.VMEM((2, rows, half), own.dtype),
            pltpu.SemaphoreType.DMA((2, half // WIDTH)),
        ],
        compiler_params=pltpu.CompilerParams(vmem_limit_bytes=49 * MIB),
        name="change",
    )(core, one, own, start)


def to_blocks_kernel(one, own, other, *outs):
    *by_y, near, far = outs
    half, per = other.shape[1], by_y[0].shape[0]
    edge = by_y[0].shape[1]
    for at in range(0, half, WIDTH):
        here = slice(at, at + WIDTH)
        s = own[:, here] - jnp.dot(one[...], other[:, here], preferred_element_type=jnp.float32)
        for j in range(len(by_y)):
            block = s[j * per : (j + 1) * per]
            if at < edge:
                by_y[j][:, here] = block
            else:
                to = slice(j * per // 2, (j + 1) * per // 2), slice(at - edge, at - edge + WIDTH)
                near[to] = block[: per // 2]
                far[to] = block[per // 2 :]


def to_blocks(one, own, other, n):
    rows, half = other.shape
    shapes = [(rows // n, half // 2)] * n + [(rows // 2, half // 2)] * 2
    return pl.pallas_call(
        to_blocks_kernel,
        in_specs=[VMEM, VMEM, VMEM],
        out_specs=[VMEM] * len(shapes),
        out_shape=[jax.ShapeDtypeStruct(s, jnp.float32) for s in shapes],
        compiler_params=pltpu.CompilerParams(vmem_limit_bytes=6 * MIB),
        name="to_blocks",
    )(one, own, other)


def from_blocks_kernel(core, one, *refs):
    out = refs[-1]
    n = (len(refs) - 1) // 2
    ins = refs[: 2 * n]
    side, k = pl.program_id(0), pl.program_id(1)
    for s in range(2):
        for part in range(ins[0].shape[1] // WIDTH):

            @pl.when((side == s) & (k == part))
            def _():
                blocks = [b[:, part * WIDTH : (part + 1) * WIDTH] for b in ins[s * n : (s + 1) * n]]
                x = jnp.concatenate(blocks, axis=0)
                out[...] = jnp.dot(one[...], x, preferred_element_type=jnp.float32).astype(out.dtype)


def from_blocks(core, one, mine, theirs, quarter, out=None):
    rows, width = one.shape[0], 4 * mine[0].shape[1]
    steps = mine[0].shape[1] // WIDTH
    blocks = [*mine, *theirs]
    rest = [] if out is None else [out]
    return pl.pallas_call(
        from_blocks_kernel,
        grid_spec=pltpu.PrefetchScalarGridSpec(
            num_scalar_prefetch=1,
            grid=(2, steps),
            in_specs=[VMEM] * (1 + len(blocks)) + [HBM] * len(rest),
            out_specs=pl.BlockSpec(
                (rows, WIDTH), lambda s, k, core: (0, ((core[0] + s) % 2 * 2 + quarter) * steps + k)
            ),
        ),
        out_shape=jax.ShapeDtypeStruct((rows, width), mine[0].dtype),
        input_output_aliases={2 + len(blocks): 0} if rest else {},
        compiler_params=pltpu.CompilerParams(vmem_limit_bytes=10 * MIB),
        name="from_blocks",
    )(core, one, *blocks, *rest)


def step(local_params, snapshot, master, momentum):
    replicas, ny, nz, nx = (lax.axis_size(a) for a in (REP, "y", "z", "xh"))
    core = lax.axis_index("c")
    core1 = core.astype(jnp.int32)[None]
    local, start = local_params[0, 0], snapshot[0]
    rows, cols = local.shape
    half = cols // 2
    edge = half // 2
    far_y = (2, 1, 3)
    wire = jnp.float16

    def send(x, axis, by):
        return lax.ppermute(x, axis, shift(axis, by))

    def part(x, row, col):
        return lax.dynamic_slice(x, (row, col), (2, half), allow_negative_indices=False)

    def wide(x):
        return x.astype(jnp.float32)

    o = jnp.arange(rows)
    q, z, h, j = o % 4, o // 4 % nz, o // (4 * nz) % nx, o // (4 * nz * nx)
    to = row_of(j, h, (lax.axis_index("z") + z) % nz, q, 1)[:, None] == o[None]
    z = (lax.axis_index("z") - z) % nz
    back_y = o[:, None] == row_of(j, h, z, q, -1)[None]
    j, h = o // (4 * nz) % ny, o // (4 * nz * ny)
    back_x = o[:, None] == row_of(j, h, z, q, -1)[None]

    to = jnp.where(to, SCALE, 0.0).astype(jnp.bfloat16)
    at = (core * half, (1 - core) * half, 2 * core, 2 * (1 - core))
    local, start, to, at, core1 = lax.optimization_barrier((local, start, to, at, core1))
    other = send(pick(core1, local), "c", 1)
    *by_y, near, far = to_blocks(to, change(core1, to, local, start), other, ny)
    far, near = far.astype(wire), near.astype(wire)
    by_y = [x.astype(wire) for x in by_y]
    first, second = wide(by_y[0]), wide(near)
    second = second + wide(send(far, "xh", 1))
    for j in far_y:
        first = first + wide(send(by_y[j], "y", j))

    old, _ = lax.optimization_barrier(((master, momentum), (far, by_y[1:])))
    base = old[0][0] - outer_rate * nesterov_mu**2 * old[1][0]
    mine, theirs = part(base, 0, at[0]), part(base, 0, at[1])
    theirs = send(theirs, "c", 1)
    base = jnp.concatenate([jnp.where(core == 0, mine, theirs), jnp.where(core == 0, theirs, mine)], axis=0)
    base = lax.all_to_all(jnp.broadcast_to(base[None], (nz, 4, half)), "z", 0, 0, tiled=True)

    per = rows // (nx * ny)
    pieces = [second[j * per : (j + 1) * per] for j in range(ny)]
    second = pieces[0]
    far = send(first[per:].astype(wire), "xh", 1)
    for j in far_y:
        second = second + wide(send(pieces[j].astype(wire), "y", j))
    first = first[:per] + wide(far)

    far_z = (4, 3, 5, 2, 6, 1, 7)
    total = jnp.concatenate([first, second], axis=1).reshape(nz, 4, half)
    pieces = [total[k] for k in range(nz)]
    total = pieces[0]
    for k in far_z:
        total = total + wide(send(pieces[k].astype(wire), "z", k))
    grad = total * (1.0 / (SCALE * replicas))
    grad, base = lax.optimization_barrier((grad, base))
    grads = {k: send(grad, "z", k) for k in far_z}
    grads[0] = grad

    members = lax.axis_size(ALL)
    parts = lax.all_to_all(jnp.full((members, 1, 128), jnp.sum(grad * grad)), ALL, 0, 0, tiled=True)
    squares = jnp.sum(parts[:, 0, 0])
    elements = rows * cols * lax.axis_size("g")
    grad_rms = jnp.sqrt(squares / elements + epsilon)
    clip = jnp.minimum(1.0, clip_limit / grad_rms)

    mine = []
    for k in range(nz):
        there = lax.rem(lax.axis_index("z") + (nz - k), nz)
        there = lax.dynamic_index_in_dim(base, there, 0, keepdims=False, allow_negative_indices=False)
        mine.append((there - outer_rate * (1.0 + nesterov_mu) * (clip * grads[k])).astype(jnp.bfloat16))
    mine = jnp.concatenate(mine, axis=0)
    first, second = mine[:, :edge], mine[:, edge:]
    arrived = {j: send(second, "y", j) for j in far_y}
    second = jnp.concatenate([second] + [arrived[j] for j in range(1, ny)], axis=0)
    first = jnp.concatenate([first, send(first, "xh", 1)], axis=0)
    arrived = {j: send(first, "y", j) for j in far_y}
    mine = [first] + [arrived[j] for j in range(1, ny)]
    theirs = [send(x, "c", 1) for x in mine]
    new_params = from_blocks(core1, back_y.astype(jnp.bfloat16), mine, theirs, 0)
    mine = [second, send(second, "xh", 1)]
    theirs = [send(x, "c", 1) for x in mine]
    new_params = from_blocks(core1, back_x.astype(jnp.bfloat16), mine, theirs, 1, new_params)

    other = send(part(grad, at[3], 0), "c", 1)
    own = part(grad, at[2], 0)
    own = [jnp.where(core == 0, own, other), jnp.where(core == 0, other, own)]
    clipped = clip * jnp.concatenate(own, axis=1)[None]
    new_momentum = nesterov_mu * momentum + clipped
    new_master = master - outer_rate * (clipped + nesterov_mu * new_momentum)
    return (new_master, new_momentum, new_params[None])


def solution(mesh):
    finer = Mesh(mesh.devices.reshape(2, 8, 4, 2, mesh.shape["grp"]), ALL)
    in_specs = (
        P(REP, "g", None, None),
        P("g", None, None),
        P("g", REP, None),
        P("g", REP, None),
    )
    out_specs = (P("g", REP, None), P("g", REP, None), P("g", None, None))
    return jax.shard_map(step, mesh=finer, in_specs=in_specs, out_specs=out_specs, check_vma=False)
```

```python
import jax
import jax.numpy as jnp
from jax import lax
from jax.experimental import pallas as pl
from jax.experimental.pallas import tpu as pltpu
from jax.sharding import Mesh
from jax.sharding import PartitionSpec as P


REP = ("xh", "z", "y", "c")
ALL = ("xh", "z", "y", "c", "g")

nesterov_mu = 0.9
outer_rate = 0.7
clip_limit = 0.15
epsilon = 1e-06

SCALE = 16.0
WIDTH = 1024
MIB = 1024 * 1024
VMEM = pl.BlockSpec(memory_space=pltpu.VMEM)
SMEM = pl.BlockSpec(memory_space=pltpu.SMEM)
HBM = pl.BlockSpec(memory_space=pltpu.HBM)


def shift(axis, by):
    n = lax.axis_size(axis)
    return [(i, (i + by) % n) for i in range(n)]


def row_of(j, h, z, q, sign):
    ny, nz, nx = (lax.axis_size(a) for a in ("y", "z", "xh"))
    yd = (lax.axis_index("y") + sign * j) % ny
    xd = (lax.axis_index("xh") + h) % nx
    return ((xd * nz + z) * ny + yd) * 4 + q


def pick_kernel(core, local, out, sem):
    half = out.shape[1]
    begin = pl.multiple_of((1 - core[0]) * half, half)
    copy = pltpu.make_async_copy(local.at[:, pl.ds(begin, half)], out, sem)
    copy.start()
    copy.wait()


def pick(core, local):
    rows, cols = local.shape
    return pl.pallas_call(
        pick_kernel,
        in_specs=[SMEM, HBM],
        out_specs=VMEM,
        out_shape=jax.ShapeDtypeStruct((rows, cols // 2), local.dtype),
        scratch_shapes=[pltpu.SemaphoreType.DMA],
        compiler_params=pltpu.CompilerParams(vmem_limit_bytes=59 * MIB),
        name="pick",
    )(core, local)


def change_kernel(core, one, own, start, out, held, sems):
    _, half = out.shape
    copies = []
    for k in range(half // WIDTH):
        begin = pl.multiple_of(core[0] * half + k * WIDTH, WIDTH)
        for i, x in enumerate((own, start)):
            to = held.at[i, :, pl.ds(k * WIDTH, WIDTH)]
            copies.append(pltpu.make_async_copy(x.at[:, pl.ds(begin, WIDTH)], to, sems.at[i, k]))
    for copy in copies:
        copy.start()
    for k in range(half // WIDTH):
        copies[2 * k].wait()
        copies[2 * k + 1].wait()
        here = slice(k * WIDTH, (k + 1) * WIDTH)
        placed = [jnp.dot(one[...], held[i, :, here], preferred_element_type=jnp.float32) for i in range(2)]
        out[:, here] = 2.0 * placed[1] - placed[0]


def change(core, one, own, start):
    rows, cols = own.shape
    half = cols // 2
    return pl.pallas_call(
        change_kernel,
        in_specs=[SMEM, VMEM, HBM, HBM],
        out_specs=VMEM,
        out_shape=jax.ShapeDtypeStruct((rows, half), jnp.float32),
        scratch_shapes=[
            pltpu.VMEM((2, rows, half), own.dtype),
            pltpu.SemaphoreType.DMA((2, half // WIDTH)),
        ],
        compiler_params=pltpu.CompilerParams(vmem_limit_bytes=49 * MIB),
        name="change",
    )(core, one, own, start)


def to_blocks_kernel(one, own, other, *outs):
    half, per = other.shape[1], outs[0].shape[0]
    for at in range(0, half, WIDTH):
        here = slice(at, at + WIDTH)
        s = own[:, here] - jnp.dot(one[...], other[:, here], preferred_element_type=jnp.float32)
        for i, out in enumerate(outs):
            out[:, here] = s[i * per : (i + 1) * per]


def to_blocks(one, own, other, n):
    rows, half = other.shape
    return pl.pallas_call(
        to_blocks_kernel,
        in_specs=[VMEM, VMEM, VMEM],
        out_specs=[VMEM] * n,
        out_shape=[jax.ShapeDtypeStruct((rows // n, half), jnp.float32)] * n,
        compiler_params=pltpu.CompilerParams(vmem_limit_bytes=6 * MIB),
        name="to_blocks",
    )(one, own, other)


def from_blocks_kernel(core, one, *refs):
    out = refs[-1]
    n = (len(refs) - 1) // 2
    ins = refs[: 2 * n]
    side, k = pl.program_id(0), pl.program_id(1)
    for s in range(2):
        for part in range(ins[0].shape[1] // WIDTH):

            @pl.when((side == s) & (k == part))
            def _():
                blocks = [b[:, part * WIDTH : (part + 1) * WIDTH] for b in ins[s * n : (s + 1) * n]]
                x = jnp.concatenate(blocks, axis=0)
                out[...] = jnp.dot(one[...], x, preferred_element_type=jnp.float32).astype(out.dtype)


def from_blocks(core, one, mine, theirs, quarter, out=None):
    rows, width = one.shape[0], 4 * mine[0].shape[1]
    steps = mine[0].shape[1] // WIDTH
    blocks = [*mine, *theirs]
    rest = [] if out is None else [out]
    return pl.pallas_call(
        from_blocks_kernel,
        grid_spec=pltpu.PrefetchScalarGridSpec(
            num_scalar_prefetch=1,
            grid=(2, steps),
            in_specs=[VMEM] * (1 + len(blocks)) + [HBM] * len(rest),
            out_specs=pl.BlockSpec(
                (rows, WIDTH), lambda s, k, core: (0, ((core[0] + s) % 2 * 2 + quarter) * steps + k)
            ),
        ),
        out_shape=jax.ShapeDtypeStruct((rows, width), mine[0].dtype),
        input_output_aliases={2 + len(blocks): 0} if rest else {},
        compiler_params=pltpu.CompilerParams(vmem_limit_bytes=10 * MIB),
        name="from_blocks",
    )(core, one, *blocks, *rest)


def step(local_params, snapshot, master, momentum):
    replicas, ny, nz, nx = (lax.axis_size(a) for a in (REP, "y", "z", "xh"))
    core = lax.axis_index("c")
    core1 = core.astype(jnp.int32)[None]
    local, start = local_params[0, 0], snapshot[0]
    rows, cols = local.shape
    half = cols // 2
    edge = half // 2
    far_y = (2, 1, 3)
    wire = jnp.float16

    def send(x, axis, by):
        return lax.ppermute(x, axis, shift(axis, by))

    def send_xy(x, h, j):
        moves = [(a, (a // ny + h) % nx * ny + (a + j) % ny) for a in range(nx * ny)]
        return lax.ppermute(x, ("xh", "y"), moves)

    def part(x, row, col):
        return lax.dynamic_slice(x, (row, col), (2, half), allow_negative_indices=False)

    def wide(x):
        return x.astype(jnp.float32)

    o = jnp.arange(rows)
    q, z, j, h = o % 4, o // 4 % nz, o // (4 * nz) % ny, o // (4 * nz * ny)
    to = row_of(j, h, z, q, 1)[:, None] == o[None]
    back_x = o[:, None] == row_of(j, h, z, q, -1)[None]
    j, h = o // (4 * nz * nx), o // (4 * nz) % nx
    back_y = o[:, None] == row_of(j, h, z, q, -1)[None]

    to = jnp.where(to, SCALE, 0.0).astype(jnp.bfloat16)
    at = (core * half, (1 - core) * half, 2 * core, 2 * (1 - core))
    local, start, to, at, core1 = lax.optimization_barrier((local, start, to, at, core1))
    other = send(pick(core1, local), "c", 1)
    blocks = to_blocks(to, change(core1, to, local, start), other, nx * ny)
    away = [(h, j) for h in (1, 0) for j in (2, 1, 3, 0) if h or j]
    sent = {(h, j): blocks[h * ny + j].astype(wire) for h, j in away}
    total = blocks[0]
    for h, j in away:
        total = total + wide(send_xy(sent[h, j], h, j))

    old, _ = lax.optimization_barrier(((master, momentum), list(sent.values())))
    base = old[0][0] - outer_rate * nesterov_mu**2 * old[1][0]
    mine, theirs = part(base, 0, at[0]), part(base, 0, at[1])
    theirs = send(theirs, "c", 1)
    base = jnp.concatenate([jnp.where(core == 0, mine, theirs), jnp.where(core == 0, theirs, mine)], axis=0)

    total = total.astype(wire).reshape(nz, 4, half)
    base, total = lax.optimization_barrier((base, total))
    total = wide(lax.all_to_all(total, "z", 0, 0, tiled=True)).sum(axis=0)
    grad = total * (1.0 / (SCALE * replicas))
    members = lax.axis_size(ALL)
    parts = lax.all_to_all(jnp.full((members, 1, 128), jnp.sum(grad * grad)), ALL, 0, 0, tiled=True)
    squares = jnp.sum(parts[:, 0, 0])
    elements = rows * cols * lax.axis_size("g")
    grad_rms = jnp.sqrt(squares / elements + epsilon)
    clip = jnp.minimum(1.0, clip_limit / grad_rms)

    mine = (base - outer_rate * (1.0 + nesterov_mu) * (clip * grad)).astype(jnp.bfloat16)
    mine = lax.all_to_all(jnp.broadcast_to(mine[None], (nz, 4, half)), "z", 0, 0, tiled=True)
    mine = mine.reshape(nz * 4, half)
    first, second = mine[:, :edge], mine[:, edge:]
    arrived = {j: send(second, "y", j) for j in far_y}
    second = jnp.concatenate([second] + [arrived[j] for j in range(1, ny)], axis=0)
    first = jnp.concatenate([first, send(first, "xh", 1)], axis=0)
    arrived = {j: send(first, "y", j) for j in far_y}
    mine = [first] + [arrived[j] for j in range(1, ny)]
    theirs = [send(x, "c", 1) for x in mine]
    new_params = from_blocks(core1, back_y.astype(jnp.bfloat16), mine, theirs, 0)
    arrived = send(second, "xh", 1)
    theirs = [send(second, "c", 1)]
    arrived, new_params = lax.optimization_barrier((arrived, new_params))
    mine = [second, arrived]
    theirs.append(send(arrived, "c", 1))
    new_params = from_blocks(core1, back_x.astype(jnp.bfloat16), mine, theirs, 1, new_params)

    other = send(part(grad, at[3], 0), "c", 1)
    own = part(grad, at[2], 0)
    own = [jnp.where(core == 0, own, other), jnp.where(core == 0, other, own)]
    clipped = clip * jnp.concatenate(own, axis=1)[None]
    new_momentum = nesterov_mu * momentum + clipped
    new_master = master - outer_rate * (clipped + nesterov_mu * new_momentum)
    return (new_master, new_momentum, new_params[None])


def solution(mesh):
    finer = Mesh(mesh.devices.reshape(2, 8, 4, 2, mesh.shape["grp"]), ALL)
    in_specs = (
        P(REP, "g", None, None),
        P("g", None, None),
        P("g", REP, None),
        P("g", REP, None),
    )
    out_specs = (P("g", REP, None), P("g", REP, None), P("g", None, None))
    return jax.shard_map(step, mesh=finer, in_specs=in_specs, out_specs=out_specs, check_vma=False)
```

```python
import jax
import jax.numpy as jnp
from jax import lax
from jax.experimental import pallas as pl
from jax.experimental.pallas import tpu as pltpu
from jax.sharding import Mesh
from jax.sharding import PartitionSpec as P


REP = ("xh", "z", "y", "c")
ALL = ("xh", "z", "y", "c", "g")

nesterov_mu = 0.9
outer_rate = 0.7
clip_limit = 0.15
epsilon = 1e-06

SCALE = 16.0
WIDTH = 1024
MIB = 1024 * 1024
VMEM = pl.BlockSpec(memory_space=pltpu.VMEM)
SMEM = pl.BlockSpec(memory_space=pltpu.SMEM)
HBM = pl.BlockSpec(memory_space=pltpu.HBM)


def shift(axis, by):
    n = lax.axis_size(axis)
    return [(i, (i + by) % n) for i in range(n)]


def row_of(j, h, z, q, sign):
    ny, nz, nx = (lax.axis_size(a) for a in ("y", "z", "xh"))
    yd = (lax.axis_index("y") + sign * j) % ny
    xd = (lax.axis_index("xh") + h) % nx
    return ((xd * nz + z) * ny + yd) * 4 + q


def pick_kernel(core, local, out, sem):
    half = out.shape[1]
    begin = pl.multiple_of((1 - core[0]) * half, half)
    copy = pltpu.make_async_copy(local.at[:, pl.ds(begin, half)], out, sem)
    copy.start()
    copy.wait()


def pick(core, local):
    rows, cols = local.shape
    return pl.pallas_call(
        pick_kernel,
        in_specs=[SMEM, HBM],
        out_specs=VMEM,
        out_shape=jax.ShapeDtypeStruct((rows, cols // 2), local.dtype),
        scratch_shapes=[pltpu.SemaphoreType.DMA],
        compiler_params=pltpu.CompilerParams(vmem_limit_bytes=59 * MIB),
        name="pick",
    )(core, local)


def change_kernel(core, one, own, start, out, held, sems):
    _, half = out.shape
    copies = []
    for k in range(half // WIDTH):
        begin = pl.multiple_of(core[0] * half + k * WIDTH, WIDTH)
        for i, x in enumerate((own, start)):
            to = held.at[i, :, pl.ds(k * WIDTH, WIDTH)]
            copies.append(pltpu.make_async_copy(x.at[:, pl.ds(begin, WIDTH)], to, sems.at[i, k]))
    for copy in copies:
        copy.start()
    for k in range(half // WIDTH):
        copies[2 * k].wait()
        copies[2 * k + 1].wait()
        here = slice(k * WIDTH, (k + 1) * WIDTH)
        placed = [jnp.dot(one[...], held[i, :, here], preferred_element_type=jnp.float32) for i in range(2)]
        out[:, here] = 2.0 * placed[1] - placed[0]


def change(core, one, own, start):
    rows, cols = own.shape
    half = cols // 2
    return pl.pallas_call(
        change_kernel,
        in_specs=[SMEM, VMEM, HBM, HBM],
        out_specs=VMEM,
        out_shape=jax.ShapeDtypeStruct((rows, half), jnp.float32),
        scratch_shapes=[
            pltpu.VMEM((2, rows, half), own.dtype),
            pltpu.SemaphoreType.DMA((2, half // WIDTH)),
        ],
        compiler_params=pltpu.CompilerParams(vmem_limit_bytes=49 * MIB),
        name="change",
    )(core, one, own, start)


def to_blocks_kernel(one, own, other, *outs):
    *by_y, near, far = outs
    half, per = other.shape[1], by_y[0].shape[0]
    edge = by_y[0].shape[1]
    for at in range(0, half, WIDTH):
        here = slice(at, at + WIDTH)
        s = own[:, here] - jnp.dot(one[...], other[:, here], preferred_element_type=jnp.float32)
        for j in range(len(by_y)):
            block = s[j * per : (j + 1) * per]
            if at < edge:
                by_y[j][:, here] = block
            else:
                to = slice(j * per // 2, (j + 1) * per // 2), slice(at - edge, at - edge + WIDTH)
                near[to] = block[: per // 2]
                far[to] = block[per // 2 :]


def to_blocks(one, own, other, n):
    rows, half = other.shape
    shapes = [(rows // n, half // 2)] * n + [(rows // 2, half // 2)] * 2
    return pl.pallas_call(
        to_blocks_kernel,
        in_specs=[VMEM, VMEM, VMEM],
        out_specs=[VMEM] * len(shapes),
        out_shape=[jax.ShapeDtypeStruct(s, jnp.float32) for s in shapes],
        compiler_params=pltpu.CompilerParams(vmem_limit_bytes=6 * MIB),
        name="to_blocks",
    )(one, own, other)


def from_blocks_kernel(core, one, *refs):
    out = refs[-1]
    n = (len(refs) - 1) // 2
    ins = refs[: 2 * n]
    side, k = pl.program_id(0), pl.program_id(1)
    for s in range(2):
        for part in range(ins[0].shape[1] // WIDTH):

            @pl.when((side == s) & (k == part))
            def _():
                blocks = [b[:, part * WIDTH : (part + 1) * WIDTH] for b in ins[s * n : (s + 1) * n]]
                x = jnp.concatenate(blocks, axis=0)
                out[...] = jnp.dot(one[...], x, preferred_element_type=jnp.float32).astype(out.dtype)


def from_blocks(core, one, mine, theirs, quarter, out=None):
    rows, width = one.shape[0], 4 * mine[0].shape[1]
    steps = mine[0].shape[1] // WIDTH
    blocks = [*mine, *theirs]
    rest = [] if out is None else [out]
    return pl.pallas_call(
        from_blocks_kernel,
        grid_spec=pltpu.PrefetchScalarGridSpec(
            num_scalar_prefetch=1,
            grid=(2, steps),
            in_specs=[VMEM] * (1 + len(blocks)) + [HBM] * len(rest),
            out_specs=pl.BlockSpec(
                (rows, WIDTH), lambda s, k, core: (0, ((core[0] + s) % 2 * 2 + quarter) * steps + k)
            ),
        ),
        out_shape=jax.ShapeDtypeStruct((rows, width), mine[0].dtype),
        input_output_aliases={2 + len(blocks): 0} if rest else {},
        compiler_params=pltpu.CompilerParams(vmem_limit_bytes=10 * MIB),
        name="from_blocks",
    )(core, one, *blocks, *rest)


def step(local_params, snapshot, master, momentum):
    replicas, ny, nz, nx = (lax.axis_size(a) for a in (REP, "y", "z", "xh"))
    core = lax.axis_index("c")
    core1 = core.astype(jnp.int32)[None]
    local, start = local_params[0, 0], snapshot[0]
    rows, cols = local.shape
    half = cols // 2
    edge = half // 2
    far_y = (2, 1, 3)
    wire = jnp.float16

    def send(x, axis, by):
        return lax.ppermute(x, axis, shift(axis, by))

    def part(x, row, col):
        return lax.dynamic_slice(x, (row, col), (2, half), allow_negative_indices=False)

    def wide(x):
        return x.astype(jnp.float32)

    o = jnp.arange(rows)
    q, z, h, j = o % 4, o // 4 % nz, o // (4 * nz) % nx, o // (4 * nz * nx)
    to = row_of(j, h, z, q, 1)[:, None] == o[None]
    z = (lax.axis_index("z") - z) % nz
    back_y = o[:, None] == row_of(j, h, z, q, -1)[None]
    j, h = o // (4 * nz) % ny, o // (4 * nz * ny)
    back_x = o[:, None] == row_of(j, h, z, q, -1)[None]

    to = jnp.where(to, SCALE, 0.0).astype(jnp.bfloat16)
    at = (core * half, (1 - core) * half, 2 * core, 2 * (1 - core))
    local, start, to, at, core1 = lax.optimization_barrier((local, start, to, at, core1))
    other = send(pick(core1, local), "c", 1)
    *by_y, near, far = to_blocks(to, change(core1, to, local, start), other, ny)
    far, near = far.astype(wire), near.astype(wire)
    by_y = [x.astype(wire) for x in by_y]
    first, second = wide(by_y[0]), wide(near)
    second = second + wide(send(far, "xh", 1))
    for j in far_y:
        first = first + wide(send(by_y[j], "y", j))

    old, _ = lax.optimization_barrier(((master, momentum), (far, by_y[1:])))
    base = old[0][0] - outer_rate * nesterov_mu**2 * old[1][0]
    mine, theirs = part(base, 0, at[0]), part(base, 0, at[1])
    theirs = send(theirs, "c", 1)
    base = jnp.concatenate([jnp.where(core == 0, mine, theirs), jnp.where(core == 0, theirs, mine)], axis=0)
    base = lax.all_to_all(jnp.broadcast_to(base[None], (nz, 4, half)), "z", 0, 0, tiled=True)

    per = rows // (nx * ny)
    pieces = [second[j * per : (j + 1) * per] for j in range(ny)]
    second = pieces[0]
    far = send(first[per:].astype(wire), "xh", 1)
    for j in far_y:
        second = second + wide(send(pieces[j].astype(wire), "y", j))
    first = first[:per] + wide(far)

    far_z = (4, 3, 5, 2, 6, 1, 7)
    total = jnp.concatenate([first, second], axis=1).astype(wire).reshape(nz, 4, half)
    base, total = lax.optimization_barrier((base, total))
    total = wide(lax.all_to_all(total, "z", 0, 0, tiled=True)).sum(axis=0)
    grad = total * (1.0 / (SCALE * replicas))
    grad = lax.optimization_barrier(grad)
    grads = {k: send(grad, "z", k) for k in far_z}
    grads[0] = grad

    members = lax.axis_size(ALL)
    parts = lax.all_to_all(jnp.full((members, 1, 128), jnp.sum(grad * grad)), ALL, 0, 0, tiled=True)
    squares = jnp.sum(parts[:, 0, 0])
    elements = rows * cols * lax.axis_size("g")
    grad_rms = jnp.sqrt(squares / elements + epsilon)
    clip = jnp.minimum(1.0, clip_limit / grad_rms)

    mine = []
    for k in range(nz):
        there = lax.rem(lax.axis_index("z") + (nz - k), nz)
        there = lax.dynamic_index_in_dim(base, there, 0, keepdims=False, allow_negative_indices=False)
        mine.append((there - outer_rate * (1.0 + nesterov_mu) * (clip * grads[k])).astype(jnp.bfloat16))
    mine = jnp.concatenate(mine, axis=0)
    first, second = mine[:, :edge], mine[:, edge:]
    arrived = {j: send(second, "y", j) for j in far_y}
    second = jnp.concatenate([second] + [arrived[j] for j in range(1, ny)], axis=0)
    first = jnp.concatenate([first, send(first, "xh", 1)], axis=0)
    arrived = {j: send(first, "y", j) for j in far_y}
    mine = [first] + [arrived[j] for j in range(1, ny)]
    theirs = [send(x, "c", 1) for x in mine]
    new_params = from_blocks(core1, back_y.astype(jnp.bfloat16), mine, theirs, 0)
    mine = [second, send(second, "xh", 1)]
    theirs = [send(x, "c", 1) for x in mine]
    new_params = from_blocks(core1, back_x.astype(jnp.bfloat16), mine, theirs, 1, new_params)

    other = send(part(grad, at[3], 0), "c", 1)
    own = part(grad, at[2], 0)
    own = [jnp.where(core == 0, own, other), jnp.where(core == 0, other, own)]
    clipped = clip * jnp.concatenate(own, axis=1)[None]
    new_momentum = nesterov_mu * momentum + clipped
    new_master = master - outer_rate * (clipped + nesterov_mu * new_momentum)
    return (new_master, new_momentum, new_params[None])


def solution(mesh):
    finer = Mesh(mesh.devices.reshape(2, 8, 4, 2, mesh.shape["grp"]), ALL)
    in_specs = (
        P(REP, "g", None, None),
        P("g", None, None),
        P("g", REP, None),
        P("g", REP, None),
    )
    out_specs = (P("g", REP, None), P("g", REP, None), P("g", None, None))
    return jax.shard_map(step, mesh=finer, in_specs=in_specs, out_specs=out_specs, check_vma=False)
```

```python
import jax
import jax.numpy as jnp
from jax import lax
from jax.experimental import pallas as pl
from jax.experimental.pallas import tpu as pltpu
from jax.sharding import Mesh
from jax.sharding import PartitionSpec as P


REP = ("xh", "z", "y", "c")
ALL = ("xh", "z", "y", "c", "g")

nesterov_mu = 0.9
outer_rate = 0.7
clip_limit = 0.15
epsilon = 1e-06

SCALE = 16.0
WIDTH = 1024
MIB = 1024 * 1024
VMEM = pl.BlockSpec(memory_space=pltpu.VMEM)
SMEM = pl.BlockSpec(memory_space=pltpu.SMEM)
HBM = pl.BlockSpec(memory_space=pltpu.HBM)


def shift(axis, by):
    n = lax.axis_size(axis)
    return [(i, (i + by) % n) for i in range(n)]


def row_of(j, h, z, q, sign):
    ny, nz, nx = (lax.axis_size(a) for a in ("y", "z", "xh"))
    yd = (lax.axis_index("y") + sign * j) % ny
    xd = (lax.axis_index("xh") + h) % nx
    return ((xd * nz + z) * ny + yd) * 4 + q


def pick_kernel(core, local, out, sem):
    half = out.shape[1]
    begin = pl.multiple_of((1 - core[0]) * half, half)
    copy = pltpu.make_async_copy(local.at[:, pl.ds(begin, half)], out, sem)
    copy.start()
    copy.wait()


def pick(core, local):
    rows, cols = local.shape
    return pl.pallas_call(
        pick_kernel,
        in_specs=[SMEM, HBM],
        out_specs=VMEM,
        out_shape=jax.ShapeDtypeStruct((rows, cols // 2), local.dtype),
        scratch_shapes=[pltpu.SemaphoreType.DMA],
        compiler_params=pltpu.CompilerParams(vmem_limit_bytes=50 * MIB),
        name="pick",
    )(core, local)


def change_kernel(core, one, own, start, out, held, sems):
    _, half = out.shape
    copies = []
    for k in range(half // WIDTH):
        begin = pl.multiple_of(core[0] * half + k * WIDTH, WIDTH)
        for i, x in enumerate((own, start)):
            to = held.at[i, :, pl.ds(k * WIDTH, WIDTH)]
            copies.append(pltpu.make_async_copy(x.at[:, pl.ds(begin, WIDTH)], to, sems.at[i, k]))
    for copy in copies:
        copy.start()
    for k in range(half // WIDTH):
        copies[2 * k].wait()
        copies[2 * k + 1].wait()
        here = slice(k * WIDTH, (k + 1) * WIDTH)
        placed = [jnp.dot(one[...], held[i, :, here], preferred_element_type=jnp.float32) for i in range(2)]
        out[:, here] = 2.0 * placed[1] - placed[0]


def change(core, one, own, start):
    rows, cols = own.shape
    half = cols // 2
    return pl.pallas_call(
        change_kernel,
        in_specs=[SMEM, VMEM, HBM, HBM],
        out_specs=VMEM,
        out_shape=jax.ShapeDtypeStruct((rows, half), jnp.float32),
        scratch_shapes=[
            pltpu.VMEM((2, rows, half), own.dtype),
            pltpu.SemaphoreType.DMA((2, half // WIDTH)),
        ],
        compiler_params=pltpu.CompilerParams(vmem_limit_bytes=49 * MIB),
        name="change",
    )(core, one, own, start)


def to_blocks_kernel(one, own, other, *outs):
    *by_y, near, far = outs
    half, per = other.shape[1], by_y[0].shape[0]
    edge = by_y[0].shape[1]
    for at in range(0, half, WIDTH):
        here = slice(at, at + WIDTH)
        s = own[:, here] - jnp.dot(one[...], other[:, here], preferred_element_type=jnp.float32)
        for j in range(len(by_y)):
            block = s[j * per : (j + 1) * per]
            if at < edge:
                by_y[j][:, here] = block
            else:
                to = slice(j * per // 2, (j + 1) * per // 2), slice(at - edge, at - edge + WIDTH)
                near[to] = block[: per // 2]
                far[to] = block[per // 2 :]


def to_blocks(one, own, other, n):
    rows, half = other.shape
    shapes = [(rows // n, half // 2)] * n + [(rows // 2, half // 2)] * 2
    return pl.pallas_call(
        to_blocks_kernel,
        in_specs=[VMEM, VMEM, VMEM],
        out_specs=[VMEM] * len(shapes),
        out_shape=[jax.ShapeDtypeStruct(s, jnp.float32) for s in shapes],
        compiler_params=pltpu.CompilerParams(vmem_limit_bytes=6 * MIB),
        name="to_blocks",
    )(one, own, other)


def from_blocks_kernel(core, one, *refs):
    out = refs[-1]
    n = (len(refs) - 1) // 2
    ins = refs[: 2 * n]
    side, k = pl.program_id(0), pl.program_id(1)
    for s in range(2):
        for part in range(ins[0].shape[1] // WIDTH):

            @pl.when((side == s) & (k == part))
            def _():
                blocks = [b[:, part * WIDTH : (part + 1) * WIDTH] for b in ins[s * n : (s + 1) * n]]
                x = jnp.concatenate(blocks, axis=0)
                out[...] = jnp.dot(one[...], x, preferred_element_type=jnp.float32).astype(out.dtype)


def from_blocks(core, one, mine, theirs, quarter, out=None):
    rows, width = one.shape[0], 4 * mine[0].shape[1]
    steps = mine[0].shape[1] // WIDTH
    blocks = [*mine, *theirs]
    rest = [] if out is None else [out]
    return pl.pallas_call(
        from_blocks_kernel,
        grid_spec=pltpu.PrefetchScalarGridSpec(
            num_scalar_prefetch=1,
            grid=(2, steps),
            in_specs=[VMEM] * (1 + len(blocks)) + [HBM] * len(rest),
            out_specs=pl.BlockSpec(
                (rows, WIDTH), lambda s, k, core: (0, ((core[0] + s) % 2 * 2 + quarter) * steps + k)
            ),
        ),
        out_shape=jax.ShapeDtypeStruct((rows, width), mine[0].dtype),
        input_output_aliases={2 + len(blocks): 0} if rest else {},
        compiler_params=pltpu.CompilerParams(vmem_limit_bytes=10 * MIB),
        name="from_blocks",
    )(core, one, *blocks, *rest)


def step(local_params, snapshot, master, momentum):
    replicas, ny, nz, nx = (lax.axis_size(a) for a in (REP, "y", "z", "xh"))
    core = lax.axis_index("c")
    core1 = core.astype(jnp.int32)[None]
    local, start = local_params[0, 0], snapshot[0]
    rows, cols = local.shape
    half = cols // 2
    edge = half // 2
    far_y = (2, 1, 3)
    wire = jnp.float16

    def send(x, axis, by):
        return lax.ppermute(x, axis, shift(axis, by))

    def part(x, row, col):
        return lax.dynamic_slice(x, (row, col), (2, half), allow_negative_indices=False)

    def wide(x):
        return x.astype(jnp.float32)

    o = jnp.arange(rows)
    q, z, h, j = o % 4, o // 4 % nz, o // (4 * nz) % nx, o // (4 * nz * nx)
    to = row_of(j, h, z, q, 1)[:, None] == o[None]
    z = (lax.axis_index("z") - z) % nz
    back_y = o[:, None] == row_of(j, h, z, q, -1)[None]
    j, h = o // (4 * nz) % ny, o // (4 * nz * ny)
    back_x = o[:, None] == row_of(j, h, z, q, -1)[None]

    to = jnp.where(to, SCALE, 0.0).astype(jnp.bfloat16)
    at = (core * half, (1 - core) * half, 2 * core, 2 * (1 - core))
    local, start, to, at, core1 = lax.optimization_barrier((local, start, to, at, core1))
    other = send(pick(core1, local), "c", 1)
    *by_y, near, far = to_blocks(to, change(core1, to, local, start), other, ny)
    far, near = far.astype(wire), near.astype(wire)
    by_y = [x.astype(wire) for x in by_y]
    first, second = wide(by_y[0]), wide(near)
    second = second + wide(send(far, "xh", 1))
    for j in far_y:
        first = first + wide(send(by_y[j], "y", j))

    old, _ = lax.optimization_barrier(((master, momentum), (far, by_y[1:])))
    base = old[0][0] - outer_rate * nesterov_mu**2 * old[1][0]
    mine, theirs = part(base, 0, at[0]), part(base, 0, at[1])
    theirs = send(theirs, "c", 1)
    base = jnp.concatenate([jnp.where(core == 0, mine, theirs), jnp.where(core == 0, theirs, mine)], axis=0)
    base = lax.all_to_all(jnp.broadcast_to(base[None], (nz, 4, half)), "z", 0, 0, tiled=True)

    per = rows // (nx * ny)
    pieces = [second[j * per : (j + 1) * per] for j in range(ny)]
    second = pieces[0]
    far = send(first[per:].astype(wire), "xh", 1)
    for j in far_y:
        second = second + wide(send(pieces[j].astype(wire), "y", j))
    first = first[:per] + wide(far)

    far_z = (4, 3, 5, 2, 6, 1, 7)
    total = jnp.concatenate([first, second], axis=1).astype(wire).reshape(nz, 4, half)
    base, total = lax.optimization_barrier((base, total))
    total = wide(lax.all_to_all(total, "z", 0, 0, tiled=True)).sum(axis=0)
    grad = total * (1.0 / (SCALE * replicas))
    grad = lax.optimization_barrier(grad)
    grads = {k: send(grad, "z", k) for k in far_z}
    grads[0] = grad

    members = lax.axis_size(ALL)
    parts = lax.all_to_all(jnp.full((members, 1, 128), jnp.sum(grad * grad)), ALL, 0, 0, tiled=True)
    squares = jnp.sum(parts[:, 0, 0])
    elements = rows * cols * lax.axis_size("g")
    grad_rms = jnp.sqrt(squares / elements + epsilon)
    clip = jnp.minimum(1.0, clip_limit / grad_rms)

    mine = []
    for k in range(nz):
        there = lax.rem(lax.axis_index("z") + (nz - k), nz)
        there = lax.dynamic_index_in_dim(base, there, 0, keepdims=False, allow_negative_indices=False)
        mine.append((there - outer_rate * (1.0 + nesterov_mu) * (clip * grads[k])).astype(jnp.bfloat16))
    mine = jnp.concatenate(mine, axis=0)
    first, second = mine[:, :edge], mine[:, edge:]
    arrived = {j: send(second, "y", j) for j in far_y}
    second = jnp.concatenate([second] + [arrived[j] for j in range(1, ny)], axis=0)
    first = jnp.concatenate([first, send(first, "xh", 1)], axis=0)
    mine = [second, send(second, "xh", 1)]
    theirs = [send(x, "c", 1) for x in mine]
    new_params = from_blocks(core1, back_x.astype(jnp.bfloat16), mine, theirs, 1)
    arrived = {j: send(first, "y", j) for j in far_y}
    arrived, new_params = lax.optimization_barrier((arrived, new_params))
    mine = [first] + [arrived[j] for j in range(1, ny)]
    theirs = [send(x, "c", 1) for x in mine]
    new_params = from_blocks(core1, back_y.astype(jnp.bfloat16), mine, theirs, 0, new_params)

    other = send(part(grad, at[3], 0), "c", 1)
    own = part(grad, at[2], 0)
    own = [jnp.where(core == 0, own, other), jnp.where(core == 0, other, own)]
    clipped = clip * jnp.concatenate(own, axis=1)[None]
    new_momentum = nesterov_mu * momentum + clipped
    new_master = master - outer_rate * (clipped + nesterov_mu * new_momentum)
    return (new_master, new_momentum, new_params[None])


def solution(mesh):
    finer = Mesh(mesh.devices.reshape(2, 8, 4, 2, mesh.shape["grp"]), ALL)
    in_specs = (
        P(REP, "g", None, None),
        P("g", None, None),
        P("g", REP, None),
        P("g", REP, None),
    )
    out_specs = (P("g", REP, None), P("g", REP, None), P("g", None, None))
    return jax.shard_map(step, mesh=finer, in_specs=in_specs, out_specs=out_specs, check_vma=False)
```

```python
import jax
import jax.numpy as jnp
from jax import lax
from jax.experimental import pallas as pl
from jax.experimental.pallas import tpu as pltpu
from jax.sharding import Mesh
from jax.sharding import PartitionSpec as P


REP = ("xh", "z", "y", "c")
ALL = ("xh", "z", "y", "c", "g")

nesterov_mu = 0.9
outer_rate = 0.7
clip_limit = 0.15
epsilon = 1e-06

SCALE = 16.0
WIDTH = 1024
STEP = 512
MIB = 1024 * 1024
VMEM = pl.BlockSpec(memory_space=pltpu.VMEM)
SMEM = pl.BlockSpec(memory_space=pltpu.SMEM)
HBM = pl.BlockSpec(memory_space=pltpu.HBM)


def shift(axis, by):
    n = lax.axis_size(axis)
    return [(i, (i + by) % n) for i in range(n)]


def row_of(j, h, z, q, sign):
    ny, nz, nx = (lax.axis_size(a) for a in ("y", "z", "xh"))
    yd = (lax.axis_index("y") + sign * j) % ny
    xd = (lax.axis_index("xh") + h) % nx
    return ((xd * nz + z) * ny + yd) * 4 + q


def pick_kernel(core, local, out, sem):
    half = out.shape[1]
    begin = pl.multiple_of((1 - core[0]) * half, half)
    copy = pltpu.make_async_copy(local.at[:, pl.ds(begin, half)], out, sem)
    copy.start()
    copy.wait()


def pick(core, local):
    rows, cols = local.shape
    return pl.pallas_call(
        pick_kernel,
        in_specs=[SMEM, HBM],
        out_specs=VMEM,
        out_shape=jax.ShapeDtypeStruct((rows, cols // 2), local.dtype),
        scratch_shapes=[pltpu.SemaphoreType.DMA],
        compiler_params=pltpu.CompilerParams(vmem_limit_bytes=50 * MIB),
        name="pick",
    )(core, local)


def change_kernel(core, one, own, start, out, held, sems):
    _, half = out.shape
    copies = []
    for k in range(half // WIDTH):
        begin = pl.multiple_of(core[0] * half + k * WIDTH, WIDTH)
        for i, x in enumerate((own, start)):
            to = held.at[i, :, pl.ds(k * WIDTH, WIDTH)]
            copies.append(pltpu.make_async_copy(x.at[:, pl.ds(begin, WIDTH)], to, sems.at[i, k]))
    for copy in copies:
        copy.start()
    for k in range(half // WIDTH):
        copies[2 * k].wait()
        copies[2 * k + 1].wait()
        here = slice(k * WIDTH, (k + 1) * WIDTH)
        placed = [jnp.dot(one[...], held[i, :, here], preferred_element_type=jnp.float32) for i in range(2)]
        out[:, here] = 2.0 * placed[1] - placed[0]


def change(core, one, own, start):
    rows, cols = own.shape
    half = cols // 2
    return pl.pallas_call(
        change_kernel,
        in_specs=[SMEM, VMEM, HBM, HBM],
        out_specs=VMEM,
        out_shape=jax.ShapeDtypeStruct((rows, half), jnp.float32),
        scratch_shapes=[
            pltpu.VMEM((2, rows, half), own.dtype),
            pltpu.SemaphoreType.DMA((2, half // WIDTH)),
        ],
        compiler_params=pltpu.CompilerParams(vmem_limit_bytes=49 * MIB),
        name="change",
    )(core, one, own, start)


def to_blocks_kernel(one, own, other, *outs):
    *by_y, near, far = outs
    half, per = other.shape[1], by_y[0].shape[0]
    edge = by_y[0].shape[1]
    for at in range(0, half, WIDTH):
        here = slice(at, at + WIDTH)
        s = own[:, here] - jnp.dot(one[...], other[:, here], preferred_element_type=jnp.float32)
        for j in range(len(by_y)):
            block = s[j * per : (j + 1) * per]
            if at < edge:
                by_y[j][:, here] = block
            else:
                to = slice(j * per // 2, (j + 1) * per // 2), slice(at - edge, at - edge + WIDTH)
                near[to] = block[: per // 2]
                far[to] = block[per // 2 :]


def to_blocks(one, own, other, n):
    rows, half = other.shape
    shapes = [(rows // n, half // 2)] * n + [(rows // 2, half // 2)] * 2
    return pl.pallas_call(
        to_blocks_kernel,
        in_specs=[VMEM, VMEM, VMEM],
        out_specs=[VMEM] * len(shapes),
        out_shape=[jax.ShapeDtypeStruct(s, jnp.float32) for s in shapes],
        compiler_params=pltpu.CompilerParams(vmem_limit_bytes=6 * MIB),
        name="to_blocks",
    )(one, own, other)


def from_blocks_kernel(core, one, *refs):
    out = refs[-1]
    n = (len(refs) - 1) // 2
    ins = refs[: 2 * n]
    side, k = pl.program_id(0), pl.program_id(1)
    for s in range(2):
        for part in range(ins[0].shape[1] // STEP):

            @pl.when((side == s) & (k == part))
            def _():
                blocks = [b[:, part * STEP : (part + 1) * STEP] for b in ins[s * n : (s + 1) * n]]
                x = jnp.concatenate(blocks, axis=0)
                out[...] = jnp.dot(one[...], x, preferred_element_type=jnp.float32).astype(out.dtype)


def from_blocks(core, one, mine, theirs, begin, half, out=None):
    rows, width = one.shape[0], 2 * half
    steps = mine[0].shape[1] // STEP
    blocks = [*mine, *theirs]
    rest = [] if out is None else [out]
    return pl.pallas_call(
        from_blocks_kernel,
        grid_spec=pltpu.PrefetchScalarGridSpec(
            num_scalar_prefetch=1,
            grid=(2, steps),
            in_specs=[VMEM] * (1 + len(blocks)) + [HBM] * len(rest),
            out_specs=pl.BlockSpec(
                (rows, STEP), lambda s, k, core: (0, ((core[0] + s) % 2 * half + begin) // STEP + k)
            ),
        ),
        out_shape=jax.ShapeDtypeStruct((rows, width), mine[0].dtype),
        input_output_aliases={2 + len(blocks): 0} if rest else {},
        compiler_params=pltpu.CompilerParams(vmem_limit_bytes=10 * MIB),
        name="from_blocks",
    )(core, one, *blocks, *rest)


def step(local_params, snapshot, master, momentum):
    replicas, ny, nz, nx = (lax.axis_size(a) for a in (REP, "y", "z", "xh"))
    core = lax.axis_index("c")
    core1 = core.astype(jnp.int32)[None]
    local, start = local_params[0, 0], snapshot[0]
    rows, cols = local.shape
    half = cols // 2
    edge = half // 2
    far_y = (2, 1, 3)
    wire = jnp.float16

    def send(x, axis, by):
        return lax.ppermute(x, axis, shift(axis, by))

    def part(x, row, col):
        return lax.dynamic_slice(x, (row, col), (2, half), allow_negative_indices=False)

    def wide(x):
        return x.astype(jnp.float32)

    o = jnp.arange(rows)
    q, z, h, j = o % 4, o // 4 % nz, o // (4 * nz) % nx, o // (4 * nz * nx)
    to = row_of(j, h, z, q, 1)[:, None] == o[None]
    z = (lax.axis_index("z") - z) % nz
    back_y = o[:, None] == row_of(j, h, z, q, -1)[None]
    j, h = o // (4 * nz) % ny, o // (4 * nz * ny)
    back_x = o[:, None] == row_of(j, h, z, q, -1)[None]

    to = jnp.where(to, SCALE, 0.0).astype(jnp.bfloat16)
    at = (core * half, (1 - core) * half, 2 * core, 2 * (1 - core))
    local, start, to, at, core1 = lax.optimization_barrier((local, start, to, at, core1))
    other = send(pick(core1, local), "c", 1)
    *by_y, near, far = to_blocks(to, change(core1, to, local, start), other, ny)
    far, near = far.astype(wire), near.astype(wire)
    by_y = [x.astype(wire) for x in by_y]
    first, second = wide(by_y[0]), wide(near)
    second = second + wide(send(far, "xh", 1))
    for j in far_y:
        first = first + wide(send(by_y[j], "y", j))

    old, _ = lax.optimization_barrier(((master, momentum), (far, by_y[1:])))
    base = old[0][0] - outer_rate * nesterov_mu**2 * old[1][0]
    mine, theirs = part(base, 0, at[0]), part(base, 0, at[1])
    theirs = send(theirs, "c", 1)
    base = jnp.concatenate([jnp.where(core == 0, mine, theirs), jnp.where(core == 0, theirs, mine)], axis=0)
    base = lax.all_to_all(jnp.broadcast_to(base[None], (nz, 4, half)), "z", 0, 0, tiled=True)

    per = rows // (nx * ny)
    pieces = [second[j * per : (j + 1) * per] for j in range(ny)]
    second = pieces[0]
    far = send(first[per:].astype(wire), "xh", 1)
    for j in far_y:
        second = second + wide(send(pieces[j].astype(wire), "y", j))
    first = first[:per] + wide(far)

    far_z = (4, 3, 5, 2, 6, 1, 7)
    total = jnp.concatenate([first, second], axis=1).astype(wire).reshape(nz, 4, half)
    base, total = lax.optimization_barrier((base, total))
    total = wide(lax.all_to_all(total, "z", 0, 0, tiled=True)).sum(axis=0)
    grad = total * (1.0 / (SCALE * replicas))
    grad = lax.optimization_barrier(grad)
    grads = {k: send(grad, "z", k) for k in far_z}
    grads[0] = grad

    members = lax.axis_size(ALL)
    parts = lax.all_to_all(jnp.full((members, 1, 128), jnp.sum(grad * grad)), ALL, 0, 0, tiled=True)
    squares = jnp.sum(parts[:, 0, 0])
    elements = rows * cols * lax.axis_size("g")
    grad_rms = jnp.sqrt(squares / elements + epsilon)
    clip = jnp.minimum(1.0, clip_limit / grad_rms)

    mine = []
    for k in range(nz):
        there = lax.rem(lax.axis_index("z") + (nz - k), nz)
        there = lax.dynamic_index_in_dim(base, there, 0, keepdims=False, allow_negative_indices=False)
        mine.append((there - outer_rate * (1.0 + nesterov_mu) * (clip * grads[k])).astype(jnp.bfloat16))
    mine = jnp.concatenate(mine, axis=0)
    edge = half * 3 // 8
    first, second = mine[:, :edge], mine[:, edge:]
    arrived = {j: send(second, "y", j) for j in far_y}
    second = jnp.concatenate([second] + [arrived[j] for j in range(1, ny)], axis=0)
    first = jnp.concatenate([first, send(first, "xh", 1)], axis=0)
    mine = [second, send(second, "xh", 1)]
    theirs = [send(x, "c", 1) for x in mine]
    new_params = from_blocks(core1, back_x.astype(jnp.bfloat16), mine, theirs, edge, half)
    arrived = {j: send(first, "y", j) for j in far_y}
    arrived, new_params = lax.optimization_barrier((arrived, new_params))
    mine = [first] + [arrived[j] for j in range(1, ny)]
    theirs = [send(x, "c", 1) for x in mine]
    new_params = from_blocks(core1, back_y.astype(jnp.bfloat16), mine, theirs, 0, half, new_params)

    other = send(part(grad, at[3], 0), "c", 1)
    own = part(grad, at[2], 0)
    own = [jnp.where(core == 0, own, other), jnp.where(core == 0, other, own)]
    clipped = clip * jnp.concatenate(own, axis=1)[None]
    new_momentum = nesterov_mu * momentum + clipped
    new_master = master - outer_rate * (clipped + nesterov_mu * new_momentum)
    return (new_master, new_momentum, new_params[None])


def solution(mesh):
    finer = Mesh(mesh.devices.reshape(2, 8, 4, 2, mesh.shape["grp"]), ALL)
    in_specs = (
        P(REP, "g", None, None),
        P("g", None, None),
        P("g", REP, None),
        P("g", REP, None),
    )
    out_specs = (P("g", REP, None), P("g", REP, None), P("g", None, None))
    return jax.shard_map(step, mesh=finer, in_specs=in_specs, out_specs=out_specs, check_vma=False)
```
